1024 devices in a mesh: gx: 32 (over z), gy: 8 (over y, core), gz: 4 (over x).
Axes of the slice: x: 4, y: 4, z: 32, core: 2. Of those that a mesh axis runs over, the one named last changes fastest.
Arguments:
- coarse_source: float32 [512, 256, 512], P('gx', 'gy', 'gz'), may hold values from -6 to 6
- coarse_shift: float32 [512, 256, 512], P('gx', 'gy', 'gz'), may hold values from 0.1 to 4
- coarse_start: float32 [512, 256, 512], P('gx', 'gy', 'gz'), may hold values from -3 to 3
- fine_source: float32 [4096, 32768], P(('gx', 'gy', 'gz')), may hold values from -6 to 6
- fine_shift: float32 [4096, 32768], P(('gx', 'gy', 'gz')), may hold values from 0.1 to 4
- fine_start: float32 [4096, 32768], P(('gx', 'gy', 'gz')), may hold values from -3 to 3
- box_corner: int32 [1024, 4, 3], P(('gx', 'gy', 'gz')), may hold values from 0 to 992, as said below
- box_owner: int32 [1024, 4], P(('gx', 'gy', 'gz')), may hold values from 0 to 32, as said below
Outputs:
- potential: float32 [512, 256, 512], P('gx', 'gy', 'gz')
- fine_solution: float32 [4096, 32768], P(('gx', 'gy', 'gz'))
- residual_norms: float32 [2], replicated
The draws below stay inside these ranges and needn't reach their ends.
Inputs may be any that keep to these rules, and one draw needn't show every extreme that they name: `box_owner`: each device has at least one live slot; in every group of 32 devices that share a gx index some device has 4 live slots; the live owners of one device are distinct; no device is the owner of more than 4 live boxes, and in every group some device is the owner of exactly 4 live boxes. `box_corner`: each corner is a multiple of 32 and its footprint lies in the coarse block of the device that lists it; the 4 footprints of one device are distinct.
All inputs are finite; a program needn't handle non-finite values.
Results may differ from the reference program's by a relative error of at most 0.0001.
Values sent between devices are 32-bit elements; how exact they have to be, the bound alone decides.
A program may use at most 128 MiB of HBM per device.

```python
import math
import jax
import jax.numpy as jnp
from jax import lax

CX = 16
CY = 32
CZ = 128
FOOT = 16
SLOTS = 4
CYCLES = 2
CSWEEPS = 4
FSWEEPS = 3
FINE = 32768
BOXES = 4096
NX = 512
NY = 256
NZ = 512
N_GY = 8
N_GZ = 4
DEVICES = 1024


def draw_box_owner(key, part):
    group = N_GY * N_GZ
    keys = jax.random.split(jax.random.fold_in(key, 41), DEVICES // group)

    def choose(single):
        return jax.random.permutation(single, group)[:SLOTS].astype(jnp.int32)
    offsets = jnp.repeat(jax.vmap(choose)(keys), group, axis=0)
    heavy = jnp.repeat(jax.random.randint(jax.random.fold_in(key, 42), (DEVICES // group,), 0, group).astype(jnp.int32), group)
    counts = jax.random.randint(jax.random.fold_in(key, 11), (DEVICES,), 1, SLOTS + 1).astype(jnp.int32)
    rank = jnp.arange(DEVICES, dtype=jnp.int32) % group
    senders = (heavy[:, None] - offsets) % group
    full = jnp.any(senders == rank[:, None], axis=1)
    counts = jnp.where(full, SLOTS, counts).astype(jnp.int32)
    owners = ((rank[:, None] + offsets) % group).astype(jnp.int32)
    slot = jnp.arange(SLOTS, dtype=jnp.int32)[None, :]
    return jnp.where(slot < counts[:, None], owners, group).astype(jnp.int32)


def draw_box_corner(key, part):
    group = N_GY * N_GZ
    along_x = CX // FOOT
    along_y = CY // FOOT
    along_z = CZ // FOOT
    places = along_x * along_y * along_z
    keys = jax.random.split(jax.random.fold_in(key, 31), DEVICES)

    def choose(single):
        return jax.random.permutation(single, places)[:SLOTS].astype(jnp.int32)
    picked = jax.vmap(choose)(keys)
    device = jnp.arange(DEVICES, dtype=jnp.int32)[:, None]
    device_x = device // group
    device_y = device // N_GZ % N_GY
    device_z = device % N_GZ
    block_x = picked // (along_y * along_z)
    block_y = picked // along_z % along_y
    block_z = picked % along_z
    fine_x = 2 * (device_x * CX + block_x * FOOT)
    fine_y = 2 * (device_y * CY + block_y * FOOT)
    fine_z = 2 * (device_z * CZ + block_z * FOOT)
    return jnp.stack([fine_x, fine_y, fine_z], axis=-1).astype(jnp.int32)


def block_levels(stream_key, dims, shards, low, largest):
    loudness = 1.0
    for axis_at, blocks in shards:
        steps = jax.random.uniform(jax.random.fold_in(jax.random.fold_in(stream_key, 6), axis_at), (blocks,), jnp.float32, low / len(shards), largest / len(shards))
        loudness = loudness * jnp.repeat(jnp.exp(steps), dims[axis_at] // blocks).reshape((-1,) + (1,) * (len(dims) - 1 - axis_at))
    return loudness


def noise(rng, dims, deviation, limit, cuts=(), kind=jnp.bfloat16):
    result = jax.random.normal(rng, dims, jnp.float32) * deviation
    if len(cuts) > 0:
        result = block_levels(rng, dims, cuts, -0.22, 0.18) * result
    return jnp.clip(result, min=-limit, max=limit).astype(kind)


def setup_inputs(seed: int = 0) -> dict:
    seeds = jax.random.split(jax.random.key(seed), 9)
    coarse_source = noise(seeds[0], (NX, NY, NZ), 1.0, 6.0, ((0, 32), (1, 8), (2, 4)), jnp.float32)
    coarse_shift = jnp.clip(jnp.exp(math.log(4.0) - 3.6888794 * jax.random.uniform(seeds[1], (NX, NY, NZ), jnp.float32) ** block_levels(seeds[1], (NX, NY, NZ), ((0, 32), (1, 8), (2, 4)), -0.2, 0.2)), 0.1, 4.0)
    coarse_start = noise(seeds[2], (NX, NY, NZ), 0.5, 3.0, ((0, 32), (1, 8), (2, 4)), jnp.float32)
    fine_source = noise(seeds[3], (BOXES, FINE), 1.0, 6.0, ((0, 1024),), jnp.float32)
    fine_shift = jnp.clip(jnp.exp(math.log(4.0) - 3.6888794 * jax.random.uniform(seeds[4], (BOXES, FINE), jnp.float32) ** block_levels(seeds[4], (BOXES, FINE), ((0, 1024),), -0.2, 0.2)), 0.1, 4.0)
    fine_start = noise(seeds[5], (BOXES, FINE), 0.5, 3.0, ((0, 1024),), jnp.float32)
    box_corner = draw_box_corner(jax.random.fold_in(seeds[8], 71), 0)
    box_owner = draw_box_owner(jax.random.fold_in(seeds[8], 71), 0)
    return {"coarse_source": coarse_source, "coarse_shift": coarse_shift, "coarse_start": coarse_start, "fine_source": fine_source, "fine_shift": fine_shift, "fine_start": fine_start, "box_corner": box_corner, "box_owner": box_owner}


OMEGA = 0.8

def to_blocks(field):
    extent = field.shape
    shaped = field.reshape(extent[0] // FOOT, FOOT, extent[1] // FOOT, FOOT, extent[2] // FOOT, FOOT)
    return shaped.transpose(0, 2, 4, 1, 3, 5).reshape(-1, FOOT * FOOT * FOOT)

def from_blocks(blocks, extent):
    shaped = blocks.reshape(extent[0] // FOOT, extent[1] // FOOT, extent[2] // FOOT, FOOT, FOOT, FOOT)
    return shaped.transpose(0, 3, 1, 4, 2, 5).reshape(extent)

def inject(parents):
    number = parents.shape[0]
    shaped = parents.reshape(number, FOOT, 1, FOOT, 1, FOOT, 1)
    spread = jnp.broadcast_to(shaped, (number, FOOT, 2, FOOT, 2, FOOT, 2))
    return spread.reshape(number, 8 * FOOT * FOOT * FOOT)

def restrict(values):
    number = values.shape[0]
    return values.reshape(number, FOOT, 2, FOOT, 2, FOOT, 2).mean(axis=(2, 4, 6)).reshape(number, FOOT * FOOT * FOOT)

def fine_residual(values, parents, source, shift):
    ghost = inject(parents)
    side = 2 * FOOT
    position = jnp.arange(side * side * side, dtype=jnp.int32)[None, :]
    summed = jnp.zeros_like(values)
    for stride in (1, side, side * side):
        coordinate = position // stride % side
        upper = jnp.roll(values, -stride, axis=1)
        lower = jnp.roll(values, stride, axis=1)
        summed = summed + jnp.where(coordinate < side - 1, upper, ghost) + jnp.where(coordinate > 0, lower, ghost)
    return source - (6.0 + shift) * values + summed

def beside_sum(padded):
    summed = padded[2:, 1:-1, 1:-1] + padded[:-2, 1:-1, 1:-1]
    summed = summed + padded[1:-1, 2:, 1:-1] + padded[1:-1, :-2, 1:-1]
    return summed + padded[1:-1, 1:-1, 2:] + padded[1:-1, 1:-1, :-2]

def reference(coarse_source, coarse_shift, coarse_start, fine_source, fine_shift, fine_start, box_corner, box_owner):
    group = N_GY * N_GZ
    device_ids = jnp.arange(DEVICES, dtype=jnp.int32)
    live = box_owner < group
    owner_safe = jnp.minimum(box_owner, group - 1).astype(jnp.int32)
    hit = ((box_owner[:, :, None] == jnp.arange(group, dtype=jnp.int32)[None, None, :]) & live[:, :, None]).astype(jnp.int32)
    incoming = lax.optimization_barrier(jnp.sum(hit, axis=1)).astype(jnp.int32)
    grouped = incoming.reshape(DEVICES // group, group, group)
    before = (jnp.cumsum(grouped, axis=1).astype(jnp.int32) - grouped).reshape(DEVICES, group).astype(jnp.int32)
    slot_j = jnp.take_along_axis(before, owner_safe, axis=1).astype(jnp.int32)
    owner_global = ((device_ids // group)[:, None] * group + owner_safe).astype(jnp.int32)
    rows = (owner_global * SLOTS + slot_j).astype(jnp.int32)
    targets = jnp.where(live, rows, BOXES).reshape(-1).astype(jnp.int32)
    block = (box_corner // 2 // FOOT).reshape(-1, 3)
    block_index = ((block[:, 0] * (NY // FOOT) + block[:, 1]) * (NZ // FOOT) + block[:, 2]).astype(jnp.int32)
    home_of_row = jnp.zeros((BOXES,), jnp.int32).at[targets].set(jnp.arange(DEVICES * SLOTS, dtype=jnp.int32), mode='drop')
    occupied = jnp.zeros((BOXES,), jnp.float32).at[targets].set(1.0, mode='drop')[:, None]
    row_block = block_index[home_of_row].astype(jnp.int32)
    source = fine_source
    shift = fine_shift
    values = fine_start
    fine_diagonal = 6.0 + shift
    diagonal = 6.0 + coarse_shift
    potential = coarse_start
    earlier = None
    norms = []
    for cycle in range(CYCLES):
        parents = to_blocks(potential)[row_block]
        if cycle > 0:
            values = values + inject(parents - earlier)
        for sweep in range(FSWEEPS):
            values = values + OMEGA * fine_residual(values, parents, source, shift) / fine_diagonal
        remainder = fine_residual(values, parents, source, shift)
        restricted = restrict(remainder) * occupied
        placed = jnp.zeros((NX // FOOT * (NY // FOOT) * (NZ // FOOT), FOOT * FOOT * FOOT), jnp.float32)
        placed = placed.at[row_block].add(restricted)
        composite = coarse_source + from_blocks(placed, coarse_source.shape)
        for sweep in range(CSWEEPS):
            residual = composite - diagonal * potential + beside_sum(jnp.pad(potential, 1))
            potential = potential + OMEGA * residual / diagonal
        squares = jnp.sum(residual * residual) + jnp.sum(occupied * remainder * remainder)
        norms.append(jnp.sqrt(squares / (NX * NY * NZ)))
        earlier = parents
    parents = to_blocks(potential)[row_block]
    fine_solution = (values + inject(parents - earlier)) * occupied
    return (potential, fine_solution, jnp.stack(norms))
```

```python
import functools

import jax
import jax.numpy as jnp
from jax import lax
from jax.experimental import pallas as pl
from jax.experimental.pallas import tpu as pltpu
from jax.sharding import PartitionSpec as P

FOOT = 16
CYCLES = 2
CSWEEPS = 4
FSWEEPS = 3
SLOTS = 4
OMEGA = 0.8
HIGHEST = lax.Precision.HIGHEST
F32 = jnp.float32
MESH = pl.DeviceIdType.MESH

ROWS = 512
FROWS = 1024
SWEEPS = CYCLES * CSWEEPS


def lane_roll(array, shift):
    return pltpu.roll(array, shift % 128, 1)


def group_transpose(parts):
    group = lax.broadcasted_iota(jnp.int32, (8, 128), 1) // 16
    parts = list(parts)
    for step in (1, 2, 4):
        clear = (group & step) == 0
        for i in range(8):
            if i & step:
                continue
            a, b = parts[i], parts[i + step]
            parts[i] = jnp.where(clear, a, lane_roll(b, 16 * step))
            parts[i + step] = jnp.where(clear, lane_roll(a, -16 * step), b)
    return parts


def kernel(
    sizes,
    corner,
    owner,
    source_hbm,
    shift_hbm,
    start_hbm,
    fsource_hbm,
    fshift_hbm,
    fstart_hbm,
    pot_out,
    fine_out,
    norm_out,
    pot,
    source,
    diag,
    weight,
    comp,
    xlo,
    xhi,
    ylo,
    yhi,
    zlo,
    zhi,
    yface,
    zface,
    fine,
    fsource,
    fdiag,
    fweight,
    expand,
    gather,
    dense,
    ghost,
    wide,
    packed,
    mixed,
    rblocks,
    code,
    count,
    place_of,
    flag_out,
    flag_in,
    d_out,
    d_in,
    r_out,
    r_in,
    csum,
    fsum,
    nx_in,
    np_in,
    n_send,
    local_sem,
    flag_sem,
    d_send,
    d_recv,
    r_send,
    r_recv,
    h_send,
    h_recv,
    n_sem,
    chain,
):
    n_x, n_y, n_z, cells = sizes
    members = n_y * n_z
    gx, gy, gz = lax.axis_index("gx"), lax.axis_index("gy"), lax.axis_index("gz")
    me = gy * n_z + gz

    def peer(q):
        return {"gy": q // n_z, "gz": lax.rem(q, n_z)}

    loads = [
        pltpu.make_async_copy(start_hbm, pot.at[0], local_sem.at[0]),
        pltpu.make_async_copy(source_hbm, source, local_sem.at[1]),
        pltpu.make_async_copy(shift_hbm, diag, local_sem.at[2]),
        pltpu.make_async_copy(fsource_hbm, fsource, local_sem.at[3]),
        pltpu.make_async_copy(fshift_hbm, fdiag, local_sem.at[4]),
        pltpu.make_async_copy(fstart_hbm, fine.at[0], local_sem.at[5]),
    ]
    for load in loads:
        load.start()

    barrier = pltpu.get_barrier_semaphore()

    def greet(i, carry):
        q = lax.rem(me + i, members)
        pl.semaphore_signal(barrier, inc=1, device_id=peer(q), device_id_type=MESH)
        return carry

    lax.fori_loop(1, members, greet, 0)

    def ring(distance):
        return lax.rem(gx + distance + n_x, n_x)

    for way in (1, -1):
        pl.semaphore_signal(barrier, inc=1, device_id={"gx": ring(way)}, device_id_type=MESH)

    owners = [owner[0, s] for s in range(SLOTS)]
    lives = [(o >= 0) & (o < members) for o in owners]
    places = [
        jnp.where(
            lives[s],
            ((corner[0, s, 1] >> 5) & 1) * 8 + ((corner[0, s, 2] >> 5) & 7),
            -1,
        )
        for s in range(SLOTS)
    ]
    for q in range(members):
        spot = jnp.int32(0)
        flag = jnp.int32(0)
        for s in range(SLOTS):
            mine = owners[s] == q
            spot = jnp.where(mine, places[s], spot)
            flag = jnp.where(mine, 1, flag)
        place_of[q] = spot
        flag_out[q] = jnp.full((1, 128), flag.astype(F32), F32)

    lane8 = lax.broadcasted_iota(jnp.int32, (8, 128), 1)
    sub8 = lax.broadcasted_iota(jnp.int32, (8, 128), 0)
    lane32 = lax.broadcasted_iota(jnp.int32, (32, 128), 1)
    row32 = lax.broadcasted_iota(jnp.int32, (32, 128), 0)
    low4 = sub8 < 4

    zeros = jnp.zeros((32, 128), F32)

    @pl.when(gx == 0)
    def _():
        for k in range(SWEEPS):
            xlo[k] = zeros

    @pl.when(gx == n_x - 1)
    def _():
        for k in range(SWEEPS):
            xhi[k] = zeros

    @pl.when(gy == 0)
    def _():
        for k in range(SWEEPS):
            ylo[k] = zeros[:16]

    @pl.when(gy == n_y - 1)
    def _():
        for k in range(SWEEPS):
            yhi[k] = zeros[:16]

    @pl.when(gz == 0)
    def _():
        for k in range(SWEEPS):
            zlo[k] = zeros[:8]

    @pl.when(gz == n_z - 1)
    def _():
        for k in range(SWEEPS):
            zhi[k] = zeros[:8]

    def halo_copies(k):
        return (
            (gx > 0, pot.at[k, pl.ds(0, 32)], xhi.at[k], 0, {"gx": ring(-1)}),
            (gx < n_x - 1, pot.at[k, pl.ds(ROWS - 32, 32)], xlo.at[k], 1, {"gx": ring(1)}),
            (gy > 0, yface.at[k, 0], yhi.at[k], 2, {"gy": lax.rem(gy + n_y - 1, n_y)}),
            (gy < n_y - 1, yface.at[k, 1], ylo.at[k], 3, {"gy": lax.rem(gy + 1, n_y)}),
            (gz > 0, zface.at[k], zhi.at[k], 4, {"gz": lax.rem(gz + n_z - 1, n_z)}),
            (gz < n_z - 1, zface.at[k], zlo.at[k], 5, {"gz": lax.rem(gz + 1, n_z)}),
        )

    def halo(k, act):
        for i, (there, src, dst, sem, device) in enumerate(halo_copies(k)):
            copy = pltpu.make_async_remote_copy(
                src_ref=src,
                dst_ref=dst,
                send_sem=h_send.at[k, sem],
                recv_sem=h_recv.at[k, sem],
                device_id=device,
                device_id_type=MESH,
            )
            if act == "recv":
                there = halo_copies(k)[i ^ 1][0]

            @pl.when(there)
            def _(copy=copy):
                if act == "start":
                    copy.start()
                elif act == "recv":
                    copy.wait_recv()
                else:
                    copy.wait_send()

    def faces_of(x, slab, k, acc):
        yface[k, 0, pl.ds(x, 1), :] = slab[0:1]
        yface[k, 1, pl.ds(x, 1), :] = slab[31:32]
        for t in range(4):
            v = x * 4 + t
            keep = (lane8 == 2 * v) | (lane8 == (2 * v - 1) % 128)
            acc = jnp.where(keep, lane_roll(slab[8 * t : 8 * t + 8], 2 * v), acc)
        return acc

    def send_parents(c):
        for x in range(16):
            slab = pot[c * CSWEEPS, pl.ds(x * 32, 32), :]
            before = pot[jnp.maximum(c - 1, 0) * CSWEEPS, pl.ds(x * 32, 32), :]
            slab = jnp.where(c > 0, slab - before, slab)
            for by in range(2):
                for y3 in range(2):
                    t = by * 2 + y3
                    mixed[pl.ds(by * 32 + x * 2 + y3, 8, stride=64), :] = slab[8 * t : 8 * t + 8]
        for by in range(2):
            for i in range(4):
                parts = [mixed[pl.ds(k * 64 + by * 32 + 8 * i, 8), :] for k in range(8)]
                for bz, part in enumerate(group_transpose(parts)):
                    packed[by * 8 + bz, pl.ds(8 * i, 8), :] = part

        d_in[c, me] = packed[place_of[me]]

        def send(i, carry):
            q = lax.rem(me + i, members)
            d_out[c, q] = packed[place_of[q]]
            pltpu.make_async_remote_copy(
                src_ref=d_out.at[c, q],
                dst_ref=d_in.at[c, me],
                send_sem=d_send.at[c],
                recv_sem=d_recv.at[c],
                device_id=peer(q),
                device_id_type=MESH,
            ).start()
            return carry

        lax.fori_loop(1, members, send, 0)

    def wait_all(buffer, sem):
        part = buffer.at[pl.ds(0, members - 1)]
        pltpu.make_async_copy(part, part, sem).wait()

    def recv_parents(c):
        wait_all(d_in.at[c], d_recv.at[c])

        def pick(r, acc):
            mark = code[r]
            acc = list(acc)
            for i in range(4):
                data = d_in[c, r, pl.ds(8 * i, 8), :]
                for j in range(SLOTS):
                    acc[j * 4 + i] = jnp.where(mark == j, data, acc[j * 4 + i])
            return tuple(acc)

        blank = jnp.zeros((8, 128), F32)
        acc = lax.fori_loop(0, members, pick, (blank,) * 16)
        for j in range(SLOTS):
            for i in range(4):
                dense[pl.ds(32 * i + j, 8, stride=4), :] = acc[j * 4 + i]
        for y2 in range(2):
            a = jnp.dot(
                dense[...], expand[:, pl.ds(256 * y2, 128)], precision=HIGHEST,
                preferred_element_type=F32,
            )
            b = jnp.dot(
                dense[...], expand[:, pl.ds(256 * y2 + 128, 128)], precision=HIGHEST,
                preferred_element_type=F32,
            )
            for x in range(16):
                ax, bx = a[8 * x : 8 * x + 8], b[8 * x : 8 * x + 8]
                ghost[pl.ds(x * 32 + y2 * 8, 8), :] = jnp.where(low4, ax, pltpu.roll(bx, 4, 0))
                ghost[pl.ds(x * 32 + 16 + y2 * 8, 8), :] = jnp.where(low4, pltpu.roll(ax, 4, 0), bx)

    fine_y = (row32 // 4) * 4 + lane32 // 32
    fine_z = lane32 % 32
    sides = (
        (fine_y == 0).astype(F32)
        + (fine_y == 31).astype(F32)
        + (fine_z == 0).astype(F32)
        + (fine_z == 31).astype(F32)
    )

    def use_parents(c):
        for X in range(32):
            g = ghost[pl.ds(X // 2 * 32, 32), :]
            times = sides + 1.0 if X in (0, 31) else sides
            fsource[pl.ds(X * 32, 32), :] = fsource[pl.ds(X * 32, 32), :] + times * g

        @pl.when(c > 0)
        def _():
            for X in range(32):
                at = lax.rem(c, 2)
                fine[at, pl.ds(X * 32, 32), :] = (
                    fine[at, pl.ds(X * 32, 32), :] + ghost[pl.ds(X // 2 * 32, 32), :]
                )

    not_first = fine_z > 0
    not_last = fine_z < 31
    first_group = lane32 < 32
    last_group = lane32 >= 96

    def beside(at, X):
        u = fine[at, pl.ds(X * 32, 32), :]
        after = jnp.where(row32 < 28, pltpu.roll(u, 28, 0), 0.0)
        prior = jnp.where(row32 >= 4, pltpu.roll(u, 4, 0), 0.0)
        total = lane_roll(jnp.where(first_group, after, u), -32)
        total = total + lane_roll(jnp.where(last_group, prior, u), 32)
        total = total + lane_roll(jnp.where(not_first, u, 0.0), -1)
        total = total + lane_roll(jnp.where(not_last, u, 0.0), 1)
        if X > 0:
            total = total + fine[at, pl.ds(X * 32 - 32, 32), :]
        if X < 31:
            total = total + fine[at, pl.ds(X * 32 + 32, 32), :]
        return u, total

    def fine_sweeps(c):
        def sweep(s, carry):
            at = lax.rem(c + s, 2)
            for X in range(32):
                u, total = beside(at, X)
                rows = pl.ds(X * 32, 32)
                fine[1 - at, rows, :] = (1.0 - OMEGA) * u + fweight[rows, :] * (fsource[rows, :] + total)
            return carry

        lax.fori_loop(0, FSWEEPS, sweep, 0)

        at = lax.rem(c + FSWEEPS, 2)
        squares = jnp.zeros((8, 128), F32)
        for x in range(16):
            both = None
            for X in (2 * x, 2 * x + 1):
                u, total = beside(at, X)
                rows = pl.ds(X * 32, 32)
                rem = fsource[rows, :] - fdiag[rows, :] * u + total
                sq = rem * rem
                squares = squares + ((sq[0:8] + sq[8:16]) + (sq[16:24] + sq[24:32]))
                both = rem if both is None else both + rem
            for y2 in range(2):
                lo = both[8 * y2 : 8 * y2 + 8]
                hi = both[16 + 8 * y2 : 24 + 8 * y2]
                wide[pl.ds(8 * x, 8), pl.ds(256 * y2, 128)] = jnp.where(low4, lo, pltpu.roll(hi, 4, 0))
                wide[pl.ds(8 * x, 8), pl.ds(256 * y2 + 128, 128)] = jnp.where(
                    low4, pltpu.roll(lo, 4, 0), hi
                )
        live = (sub8 % 4).astype(F32) < count[...]
        fsum[c] = jnp.where(live, squares, 0.0)
        dense[...] = jnp.dot(
            wide[...], gather[...], precision=HIGHEST, preferred_element_type=F32
        )
        for j in range(SLOTS):
            for i in range(4):
                rblocks[j, pl.ds(8 * i, 8), :] = dense[pl.ds(32 * i + j, 8, stride=4), :]

    def send_restricted(c):
        def block_for(r, i):
            mark = code[r]
            value = rblocks[0, pl.ds(8 * i, 8), :]
            for j in range(1, SLOTS):
                value = jnp.where(mark == j, rblocks[j, pl.ds(8 * i, 8), :], value)
            return value

        for i in range(4):
            r_in[c, me, pl.ds(8 * i, 8), :] = block_for(me, i)

        def send(i, carry):
            q = lax.rem(me + i, members)
            for part in range(4):
                r_out[c, q, pl.ds(8 * part, 8), :] = block_for(q, part)
            pltpu.make_async_remote_copy(
                src_ref=r_out.at[c, q],
                dst_ref=r_in.at[c, me],
                send_sem=r_send.at[c],
                recv_sem=r_recv.at[c],
                device_id=peer(q),
                device_id_type=MESH,
            ).start()
            return carry

        lax.fori_loop(1, members, send, 0)

    def recv_restricted(c):
        wait_all(r_in.at[c], r_recv.at[c])
        blocks = [r_in[c, jnp.clip(o, 0, members - 1)] for o in owners]
        for p in range(16):
            value = zeros
            for s in range(SLOTS):
                value = jnp.where(places[s] == p, blocks[s], value)
            packed[p] = value
        for by in range(2):
            for i in range(4):
                parts = [packed[by * 8 + bz, pl.ds(8 * i, 8), :] for bz in range(8)]
                for k, part in enumerate(group_transpose(parts)):
                    mixed[pl.ds(k * 64 + by * 32 + 8 * i, 8), :] = part
        for x in range(16):
            for t in range(4):
                rows = pl.ds(x * 32 + 8 * t, 8)
                comp[rows, :] = (
                    source[rows, :]
                    + mixed[pl.ds(t // 2 * 32 + x * 2 + t % 2, 8, stride=64), :]
                )

    first_lane = lane32 == 0
    last_lane = lane32 == 127

    def coarse_sweep(c, s):
        k = c * CSWEEPS + s
        halo(k, "recv")
        beyond = jnp.where(lane8 % 2 == 0, zhi[k], zlo[k])
        acc = jnp.zeros((8, 128), F32)
        squares = jnp.zeros((8, 128), F32)
        follow = jnp.minimum(k + 1, SWEEPS)
        for x in range(16):
            rows = pl.ds(x * 32, 32)
            p = pot[k, rows, :]
            total = pot[k, pl.ds(x * 32 - 32, 32), :] if x > 0 else xlo[k]
            total = total + (pot[k, pl.ds(x * 32 + 32, 32), :] if x < 15 else xhi[k])
            above = jnp.broadcast_to(yhi[k, pl.ds(x, 1), :], (32, 128))
            below = jnp.broadcast_to(ylo[k, pl.ds(x, 1), :], (32, 128))
            total = total + jnp.where(row32 == 31, above, pltpu.roll(p, 31, 0))
            total = total + jnp.where(row32 == 0, below, pltpu.roll(p, 1, 0))
            edge = jnp.concatenate(
                [lane_roll(beyond, -2 * (x * 4 + t)) for t in range(4)], axis=0
            )
            total = total + lane_roll(jnp.where(first_lane, edge, p), -1)
            total = total + lane_roll(jnp.where(last_lane, edge, p), 1)
            res = comp[rows, :] - diag[rows, :] * p + total
            sq = res * res
            squares = squares + ((sq[0:8] + sq[8:16]) + (sq[16:24] + sq[24:32]))
            new = p + weight[rows, :] * res
            pot[k + 1, rows, :] = new
            acc = faces_of(x, new, k + 1, acc)
        zface[k + 1] = acc
        csum[c] = squares

        @pl.when(k + 1 < SWEEPS)
        def _():
            halo(k + 1, "start")

    loads[0].wait()
    acc = jnp.zeros((8, 128), F32)
    for x in range(16):
        acc = faces_of(x, pot[0, pl.ds(x * 32, 32), :], 0, acc)
    zface[0] = acc
    pl.semaphore_wait(barrier, members + 1)

    flag_in[me] = flag_out[me]

    def send_flag(i, carry):
        q = lax.rem(me + i, members)
        pltpu.make_async_remote_copy(
            src_ref=flag_out.at[q],
            dst_ref=flag_in.at[me],
            send_sem=flag_sem.at[0],
            recv_sem=flag_sem.at[1],
            device_id=peer(q),
            device_id_type=MESH,
        ).start()
        return carry

    lax.fori_loop(1, members, send_flag, 0)
    halo(0, "start")

    rounds = []
    while 2 ** len(rounds) * 2 <= n_x // 2:
        rounds.append(2 ** len(rounds))

    def chain_step(at):
        if 0 < at <= len(rounds):
            pl.semaphore_wait(chain.at[at - 1], 2)
        if at < len(rounds):
            for way in (1, -1):
                pl.semaphore_signal(
                    chain.at[at],
                    inc=1,
                    device_id={"gx": ring(way * rounds[at])},
                    device_id_type=MESH,
                )

    chain_step(0)

    def prepare():
        i = lax.broadcasted_iota(jnp.int32, (128, 512), 0)
        n = lax.broadcasted_iota(jnp.int32, (128, 512), 1)
        lane = n % 128
        expand[...] = (i == (n // 128) * 32 + (lane // 64) * 16 + (lane % 32) // 2).astype(F32)
        n = lax.broadcasted_iota(jnp.int32, (512, 128), 0)
        o = lax.broadcasted_iota(jnp.int32, (512, 128), 1)
        lane = n % 128
        gather[...] = jnp.where(
            o == (n // 128) * 32 + (lane // 64) * 16 + (lane % 32) // 2, 0.125, 0.0
        )
        loads[2].wait()
        for x in range(16):
            rows = pl.ds(x * 32, 32)
            d = 6.0 + diag[rows, :]
            diag[rows, :] = d
            weight[rows, :] = OMEGA / d
        loads[4].wait()
        for X in range(32):
            rows = pl.ds(X * 32, 32)
            d = 6.0 + fdiag[rows, :]
            fdiag[rows, :] = d
            fweight[rows, :] = OMEGA / d
        for at in (1, 3, 5):
            loads[at].wait()
        wait_all(flag_in, flag_sem.at[1])
        before = jnp.zeros((8, 128), F32)
        for r in range(members):
            flag = jnp.broadcast_to(flag_in[r], (8, 128))
            code[r] = jnp.where(flag > 0.5, before, -1.0)
            before = before + flag
        count[...] = before

    norm_row = lax.broadcasted_iota(jnp.int32, (1, 128), 1)

    def norm_copy(src, dst, sem, device):
        return pltpu.make_async_remote_copy(
            src_ref=src,
            dst_ref=dst,
            send_sem=n_sem.at[sem],
            recv_sem=n_sem.at[sem + 1],
            device_id=device,
            device_id_type=MESH,
        )

    def send_norms():
        parts = [jnp.sum(csum[k] + fsum[k]) for k in range(CYCLES)]
        row = jnp.where(norm_row < 64, parts[0], parts[1])
        n_send[0] = row
        nx_in[gx] = row

        def send(i, carry):
            norm_copy(n_send.at[0], nx_in.at[gx], 0, {"gx": lax.rem(gx + i, n_x)}).start()
            return carry

        lax.fori_loop(1, n_x, send, 0)

    def turn_norms():
        part = nx_in.at[pl.ds(0, n_x - 1)]
        pltpu.make_async_copy(part, part, n_sem.at[1]).wait()
        row = nx_in[0]
        for r in range(1, n_x):
            row = row + nx_in[r]
        n_send[1] = row
        np_in[me] = row

        def send(i, carry):
            norm_copy(n_send.at[1], np_in.at[me], 2, peer(lax.rem(me + i, members))).start()
            return carry

        lax.fori_loop(1, members, send, 0)

    def end_norms():
        wait_all(np_in, n_sem.at[3])
        row = np_in[0]
        for r in range(1, members):
            row = row + np_in[r]
        norm_out[...] = jnp.sqrt(row / cells)

    def cycle(c, carry):
        @pl.when(c == CYCLES)
        def _():
            send_norms()

        send_parents(c)

        @pl.when(c == 0)
        def _():
            prepare()

        recv_parents(c)

        @pl.when(c < CYCLES)
        def _():
            use_parents(c)
            for k in range(CYCLES):

                @pl.when(c == k)
                def _(k=k):
                    chain_step(2 * k + 1)

            fine_sweeps(c)
            send_restricted(c)
            for k in range(CYCLES):

                @pl.when(c == k)
                def _(k=k):
                    chain_step(2 * k + 2)

            recv_restricted(c)

            def sweep(s, carry):
                coarse_sweep(c, s)
                return carry

            lax.fori_loop(0, CSWEEPS, sweep, 0)

        return carry

    lax.fori_loop(0, CYCLES + 1, cycle, 0)

    out_pot = pltpu.make_async_copy(pot.at[SWEEPS], pot_out, local_sem.at[0])
    out_pot.start()
    live = ((row32 % 4).astype(F32) < jnp.concatenate([count[...]] * 4, axis=0)).astype(F32)
    end = CYCLES % 2
    for X in range(32):
        rows = pl.ds(X * 32, 32)
        fine[1 - end, rows, :] = (fine[end, rows, :] + ghost[pl.ds(X // 2 * 32, 32), :]) * live
    out_fine = pltpu.make_async_copy(fine.at[1 - end], fine_out, local_sem.at[1])
    out_fine.start()
    turn_norms()

    wait_all(flag_out, flag_sem.at[0])
    for c in range(CYCLES + 1):
        wait_all(d_out.at[c], d_send.at[c])
    for c in range(CYCLES):
        wait_all(r_out.at[c], r_send.at[c])

    def left(k, carry):
        halo(k, "send")
        return carry

    lax.fori_loop(0, SWEEPS, left, 0)
    part = nx_in.at[pl.ds(0, n_x - 1)]
    pltpu.make_async_copy(part, part, n_sem.at[0]).wait()
    end_norms()
    wait_all(np_in, n_sem.at[2])
    out_pot.wait()
    out_fine.wait()


def local(
    coarse_source,
    coarse_shift,
    coarse_start,
    fine_source,
    fine_shift,
    fine_start,
    box_corner,
    box_owner,
):
    n_x, n_y, n_z = (lax.axis_size(a) for a in ("gx", "gy", "gz"))
    members = n_y * n_z
    cells = float(n_x * n_y * n_z * coarse_source.size)

    def fine_rows(array):
        return array.reshape(SLOTS, 256, 128).transpose(1, 0, 2).reshape(FROWS, 128)

    hbm = pl.BlockSpec(memory_space=pltpu.HBM)
    smem = pl.BlockSpec(memory_space=pltpu.SMEM)
    vmem = pl.BlockSpec(memory_space=pltpu.VMEM)

    def buf(*shape):
        return pltpu.VMEM(shape, F32)

    sems = pltpu.SemaphoreType.DMA
    pot, fine, norms = pl.pallas_call(
        functools.partial(kernel, (n_x, n_y, n_z, cells)),
        out_shape=(
            jax.ShapeDtypeStruct((ROWS, 128), F32),
            jax.ShapeDtypeStruct((FROWS, 128), F32),
            jax.ShapeDtypeStruct((1, 128), F32),
        ),
        in_specs=[smem, smem] + [hbm] * 6,
        out_specs=(hbm, hbm, vmem),
        scratch_shapes=[
            buf(SWEEPS + 1, ROWS, 128),
            buf(ROWS, 128),
            buf(ROWS, 128),
            buf(ROWS, 128),
            buf(ROWS, 128),
            buf(SWEEPS, 32, 128),
            buf(SWEEPS, 32, 128),
            buf(SWEEPS, 16, 128),
            buf(SWEEPS, 16, 128),
            buf(SWEEPS, 8, 128),
            buf(SWEEPS, 8, 128),
            buf(SWEEPS + 1, 2, 16, 128),
            buf(SWEEPS + 1, 8, 128),
            buf(2, FROWS, 128),
            buf(FROWS, 128),
            buf(FROWS, 128),
            buf(FROWS, 128),
            buf(128, 512),
            buf(512, 128),
            buf(128, 128),
            buf(ROWS, 128),
            buf(128, 512),
            buf(16, 32, 128),
            buf(ROWS, 128),
            buf(SLOTS, 32, 128),
            buf(members, 8, 128),
            buf(8, 128),
            pltpu.SMEM((members,), jnp.int32),
            buf(members, 1, 128),
            buf(members, 1, 128),
            buf(CYCLES + 1, members, 32, 128),
            buf(CYCLES + 1, members, 32, 128),
            buf(CYCLES, members, 32, 128),
            buf(CYCLES, members, 32, 128),
            buf(CYCLES, 8, 128),
            buf(CYCLES, 8, 128),
            buf(n_x, 1, 128),
            buf(members, 1, 128),
            buf(2, 1, 128),
            sems((6,)),
            sems((2,)),
            sems((CYCLES + 1,)),
            sems((CYCLES + 1,)),
            sems((CYCLES,)),
            sems((CYCLES,)),
            sems((SWEEPS, 6)),
            sems((SWEEPS, 6)),
            sems((4,)),
            pltpu.SemaphoreType.REGULAR((4,)),
        ],
        compiler_params=pltpu.CompilerParams(
            collective_id=0, has_side_effects=True, vmem_limit_bytes=60 * 1000 * 1000
        ),
        name="cycles",
    )(
        box_corner,
        box_owner,
        coarse_source.reshape(ROWS, 128),
        coarse_shift.reshape(ROWS, 128),
        coarse_start.reshape(ROWS, 128),
        fine_rows(fine_source),
        fine_rows(fine_shift),
        fine_rows(fine_start),
    )
    fine = fine.reshape(256, SLOTS, 128).transpose(1, 0, 2).reshape(SLOTS, 256 * 128)
    return pot.reshape(coarse_source.shape), fine, norms[0, ::64]


def solution(mesh):
    every = ("gx", "gy", "gz")
    return jax.shard_map(
        local,
        mesh=mesh,
        in_specs=(
            P("gx", "gy", "gz"),
            P("gx", "gy", "gz"),
            P("gx", "gy", "gz"),
            P(every, None),
            P(every, None),
            P(every, None),
            P(every, None, None),
            P(every, None),
        ),
        out_specs=(P("gx", "gy", "gz"), P(every, None), P()),
        check_vma=False,
    )
```

```python
import functools

import jax
import jax.numpy as jnp
from jax import lax
from jax.experimental import pallas as pl
from jax.experimental.pallas import tpu as pltpu
from jax.sharding import PartitionSpec as P

FOOT = 16
CYCLES = 2
CSWEEPS = 4
FSWEEPS = 3
SLOTS = 4
OMEGA = 0.8
HIGHEST = lax.Precision.HIGHEST
F32 = jnp.float32
MESH = pl.DeviceIdType.MESH

ROWS = 512
FROWS = 1024
SWEEPS = CYCLES * CSWEEPS
GATHERED = 4


def lane_roll(array, shift):
    return pltpu.roll(array, shift % 128, 1)


def group_transpose(parts):
    group = lax.broadcasted_iota(jnp.int32, (8, 128), 1) // 16
    parts = list(parts)
    for step in (1, 2, 4):
        clear = (group & step) == 0
        for i in range(8):
            if i & step:
                continue
            a, b = parts[i], parts[i + step]
            parts[i] = jnp.where(clear, a, lane_roll(b, 16 * step))
            parts[i + step] = jnp.where(clear, lane_roll(a, -16 * step), b)
    return parts


def kernel(
    sizes,
    corner,
    owner,
    source_hbm,
    shift_hbm,
    start_hbm,
    fsource_hbm,
    fshift_hbm,
    fstart_hbm,
    pot_out,
    fine_out,
    norm_out,
    pot,
    source,
    diag,
    weight,
    comp,
    xlo,
    xhi,
    ylo,
    yhi,
    zlo,
    zhi,
    yface,
    zface,
    fine,
    fsource,
    fdiag,
    fweight,
    expand,
    gather,
    dense,
    ghost,
    wide,
    packed,
    mixed,
    rblocks,
    code,
    count,
    place_of,
    slot_of,
    flag_of,
    surf,
    s_out,
    s_in,
    d_out,
    d_in,
    r_out,
    r_in,
    csum,
    fsum,
    nx_in,
    np_in,
    n_send,
    local_sem,
    s_sem,
    d_send,
    d_recv,
    r_send,
    r_recv,
    h_send,
    h_recv,
    n_sem,
    chain,
):
    n_x, n_y, n_z, cells = sizes
    members = n_y * n_z
    gx, gy, gz = lax.axis_index("gx"), lax.axis_index("gy"), lax.axis_index("gz")
    me = gy * n_z + gz

    def peer(q):
        return {"gy": q // n_z, "gz": lax.rem(q, n_z)}

    loads = [
        pltpu.make_async_copy(start_hbm, pot.at[0], local_sem.at[0]),
        pltpu.make_async_copy(source_hbm, source, local_sem.at[1]),
        pltpu.make_async_copy(shift_hbm, diag, local_sem.at[2]),
        pltpu.make_async_copy(fsource_hbm, fsource, local_sem.at[3]),
        pltpu.make_async_copy(fshift_hbm, fdiag, local_sem.at[4]),
        pltpu.make_async_copy(fstart_hbm, fine.at[0], local_sem.at[5]),
    ]
    for load in loads:
        load.start()

    barrier = pltpu.get_barrier_semaphore()

    def greet(i, carry):
        q = lax.rem(me + i, members)
        pl.semaphore_signal(barrier, inc=1, device_id=peer(q), device_id_type=MESH)
        return carry

    lax.fori_loop(1, members, greet, 0)

    def ring(distance):
        return lax.rem(gx + distance + n_x, n_x)

    for way in (1, -1):
        pl.semaphore_signal(barrier, inc=1, device_id={"gx": ring(way)}, device_id_type=MESH)

    owners = [owner[0, s] for s in range(SLOTS)]
    lives = [(o >= 0) & (o < members) for o in owners]
    places = [
        jnp.where(
            lives[s],
            ((corner[1, 0, s] >> 5) & 1) * 8 + ((corner[2, 0, s] >> 5) & 7),
            -1,
        )
        for s in range(SLOTS)
    ]
    for q in range(members):
        spot = jnp.int32(0)
        slot = jnp.int32(0)
        flag = jnp.int32(0)
        for s in range(SLOTS):
            mine = owners[s] == q
            spot = jnp.where(mine, places[s], spot)
            slot = jnp.where(mine, s, slot)
            flag = jnp.where(mine, 1, flag)
        place_of[q] = spot
        slot_of[q] = slot
        flag_of[q] = flag

    lane8 = lax.broadcasted_iota(jnp.int32, (8, 128), 1)
    sub8 = lax.broadcasted_iota(jnp.int32, (8, 128), 0)
    lane32 = lax.broadcasted_iota(jnp.int32, (32, 128), 1)
    row32 = lax.broadcasted_iota(jnp.int32, (32, 128), 0)
    low4 = sub8 < 4

    zeros = jnp.zeros((32, 128), F32)

    def halo(k, sides, act):
        routes = (
            (pot.at[k, pl.ds(0, 32)], xhi.at[k], {"gx": ring(-1)}),
            (pot.at[k, pl.ds(ROWS - 32, 32)], xlo.at[k], {"gx": ring(1)}),
            (yface.at[k, 0], yhi.at[k], {"gy": lax.rem(gy + n_y - 1, n_y)}),
            (yface.at[k, 1], ylo.at[k], {"gy": lax.rem(gy + 1, n_y)}),
            (zface.at[k], zhi.at[k], {"gz": lax.rem(gz + n_z - 1, n_z)}),
            (zface.at[k], zlo.at[k], {"gz": lax.rem(gz + 1, n_z)}),
        )
        for i in sides:
            src, dst, device = routes[i]
            copy = pltpu.make_async_remote_copy(
                src_ref=src,
                dst_ref=dst,
                send_sem=h_send.at[k, i],
                recv_sem=h_recv.at[k, i],
                device_id=device,
                device_id_type=MESH,
            )
            if act == "start":
                copy.start()
            elif act == "recv":
                copy.wait_recv()
            else:
                copy.wait_send()

    def faces_of(x, slab, k, acc):
        yface[k, 0, pl.ds(x, 1), :] = slab[0:1]
        yface[k, 1, pl.ds(x, 1), :] = slab[31:32]
        for t in range(4):
            v = x * 4 + t
            keep = (lane8 == 2 * v) | (lane8 == (2 * v - 1) % 128)
            acc = jnp.where(keep, lane_roll(slab[8 * t : 8 * t + 8], 2 * v), acc)
        return acc

    def pack_parents(slab_of):
        for x in range(16):
            slab = slab_of(x)
            for by in range(2):
                for y3 in range(2):
                    t = by * 2 + y3
                    mixed[pl.ds(by * 32 + x * 2 + y3, 8, stride=64), :] = slab[8 * t : 8 * t + 8]
        for by in range(2):
            for i in range(4):
                parts = [mixed[pl.ds(k * 64 + by * 32 + 8 * i, 8), :] for k in range(8)]
                for bz, part in enumerate(group_transpose(parts)):
                    packed[by * 8 + bz, pl.ds(8 * i, 8), :] = part

    def send_parents(c):
        rows_of = lambda at, x: pot[at, pl.ds(x * 32, 32), :]
        pack_parents(lambda x: rows_of(c * CSWEEPS + CSWEEPS, x) - rows_of(c * CSWEEPS, x))
        d_in[c, me] = packed[place_of[me]]

        def send(i, carry):
            q = lax.rem(me + members - i, members)
            d_out[c, q] = packed[place_of[q]]
            pltpu.make_async_remote_copy(
                src_ref=d_out.at[c, q],
                dst_ref=d_in.at[c, me],
                send_sem=d_send.at[c],
                recv_sem=d_recv.at[c],
                device_id=peer(q),
                device_id_type=MESH,
            ).start()
            return carry

        lax.fori_loop(1, members, send, 0)

    inner_lane = lambda lane, first: (lane > first) & (lane < first + 15)

    def surface_lane(o):
        m = o % 32
        at = jnp.where(m < 16, m, ((m - 16) // 2 + 1) * 16 + (m % 2) * 15)
        return jnp.where(m < 30, at, -1)

    def stage_surfaces():
        pack_parents(lambda x: pot[0, pl.ds(x * 32, 32), :])
        i = lax.broadcasted_iota(jnp.int32, (128, 128), 0)
        o = lax.broadcasted_iota(jnp.int32, (128, 128), 1)
        choose = (i == surface_lane(o)).astype(F32)
        for s in range(SLOTS):
            block = packed[jnp.maximum(places[s], 0)]
            odd = (row32 % 2 == 1) & inner_lane(lane32, 0)
            dense[pl.ds(32 * s, 32), :] = jnp.where(odd, lane_roll(block, 16), block)
            surf[s, pl.ds(8, 2), :] = block[0:2]
            surf[s, pl.ds(10, 2), :] = block[30:32]
        ghost[pl.ds(0, 128), :] = jnp.dot(
            dense[...], choose, precision=HIGHEST, preferred_element_type=F32
        )
        for s in range(SLOTS):
            block = ghost[pl.ds(32 * s, 32), :]
            block = jnp.where(lane32 // 32 == row32 % 4, block, 0.0)
            block = block + pltpu.roll(block, 31, 0)
            block = block + pltpu.roll(block, 30, 0)
            dense[pl.ds(32 * s, 32), :] = block
            surf[s, pl.ds(0, 8), :] = dense[pl.ds(32 * s, 8, stride=4), :]

        def stage(q, carry):
            slot = slot_of[q]
            flag = jnp.full((8, 128), flag_of[q].astype(F32), F32)
            s_out[q, pl.ds(0, 8), :] = jnp.where(lane8 == 31, flag, surf[slot, pl.ds(0, 8), :])
            s_out[q, pl.ds(8, 4), :] = surf[slot, pl.ds(8, 4), :]
            return carry

        lax.fori_loop(0, members, stage, 0)
        s_in[me] = s_out[me]

    def send_surfaces():
        def send(i, carry):
            q = lax.rem(me + members - i, members)
            pltpu.make_async_remote_copy(
                src_ref=s_out.at[q],
                dst_ref=s_in.at[me],
                send_sem=s_sem.at[0],
                recv_sem=s_sem.at[1],
                device_id=peer(q),
                device_id_type=MESH,
            ).start()
            return carry

        lax.fori_loop(1, members, send, 0)

    def recv_surfaces():
        wait_all(s_in, s_sem.at[1])
        before = jnp.zeros((8, 128), F32)
        tops = [jnp.zeros((8, 128), F32)] * SLOTS
        ends = [jnp.zeros((4, 128), F32)] * SLOTS
        for r in range(members):
            top = s_in[r, pl.ds(0, 8), :]
            end = s_in[r, pl.ds(8, 4), :]
            flag = jnp.sum(jnp.where(lane8 == 31, top, 0.0), axis=1, keepdims=True)
            flag = jnp.broadcast_to(flag, (8, 128))
            mark = jnp.where(flag > 0.5, before, -1.0)
            code[r] = mark
            before = before + flag
            for j in range(SLOTS):
                tops[j] = jnp.where(mark == j, top, tops[j])
                ends[j] = jnp.where(mark[0:4] == j, end, ends[j])
        count[...] = before
        for j in range(SLOTS):
            for i in range(4):
                dense[pl.ds(4 * i + j, 8, stride=16), :] = jnp.where(
                    lane8 // 32 == i, tops[j], 0.0
                )
        i = lax.broadcasted_iota(jnp.int32, (128, 128), 0)
        o = lax.broadcasted_iota(jnp.int32, (128, 128), 1)
        place = (surface_lane(i) == o).astype(F32)
        value = jnp.dot(dense[...], place, precision=HIGHEST, preferred_element_type=F32)
        odd = ((i // 4) % 2 == 1) & inner_lane(o, 112)
        dense[...] = jnp.where(odd, lane_roll(value, 112), value)
        for j in range(SLOTS):
            for y3 in range(2):
                dense[pl.ds(y3 * 4 + j, 1), :] = ends[j][y3 : y3 + 1]
                dense[pl.ds(120 + y3 * 4 + j, 1), :] = ends[j][2 + y3 : 3 + y3]
        spread()

    def wait_all(buffer, sem):
        part = buffer.at[pl.ds(0, members - 1)]
        pltpu.make_async_copy(part, part, sem).wait()

    def recv_parents(c):
        wait_all(d_in.at[c], d_recv.at[c])

        def pick(r8, acc):
            acc = list(acc)
            for r in range(GATHERED):
                r = r8 * GATHERED + r
                mark = code[r]
                for i in range(4):
                    data = d_in[c, r, pl.ds(8 * i, 8), :]
                    for j in range(SLOTS):
                        acc[j * 4 + i] = jnp.where(mark == j, data, acc[j * 4 + i])
            return tuple(acc)

        blank = jnp.zeros((8, 128), F32)
        acc = lax.fori_loop(0, members // GATHERED, pick, (blank,) * 16)
        for j in range(SLOTS):
            for i in range(4):
                dense[pl.ds(32 * i + j, 8, stride=4), :] = acc[j * 4 + i]
        spread()

    def spread():
        for y2 in range(2):
            a = jnp.dot(
                dense[...], expand[:, pl.ds(256 * y2, 128)], precision=HIGHEST,
                preferred_element_type=F32,
            )
            b = jnp.dot(
                dense[...], expand[:, pl.ds(256 * y2 + 128, 128)], precision=HIGHEST,
                preferred_element_type=F32,
            )
            for x in range(16):
                ax, bx = a[8 * x : 8 * x + 8], b[8 * x : 8 * x + 8]
                ghost[pl.ds(x * 32 + y2 * 8, 8), :] = jnp.where(low4, ax, pltpu.roll(bx, 4, 0))
                ghost[pl.ds(x * 32 + 16 + y2 * 8, 8), :] = jnp.where(low4, pltpu.roll(ax, 4, 0), bx)

    fine_y = (row32 // 4) * 4 + lane32 // 32
    fine_z = lane32 % 32
    sides = (
        (fine_y == 0).astype(F32)
        + (fine_y == 31).astype(F32)
        + (fine_z == 0).astype(F32)
        + (fine_z == 31).astype(F32)
    )

    def use_parents(c):
        for X in range(32):
            g = ghost[pl.ds(X // 2 * 32, 32), :]
            times = sides + 1.0 if X in (0, 31) else sides
            fsource[pl.ds(X * 32, 32), :] = fsource[pl.ds(X * 32, 32), :] + times * g

        @pl.when(c > 0)
        def _():
            for X in range(32):
                at = lax.rem(c, 2)
                fine[at, pl.ds(X * 32, 32), :] = (
                    fine[at, pl.ds(X * 32, 32), :] + ghost[pl.ds(X // 2 * 32, 32), :]
                )

    not_first = fine_z > 0
    not_last = fine_z < 31
    first_group = lane32 < 32
    last_group = lane32 >= 96

    def beside(at, X):
        u = fine[at, pl.ds(X * 32, 32), :]
        after = jnp.where(row32 < 28, pltpu.roll(u, 28, 0), 0.0)
        prior = jnp.where(row32 >= 4, pltpu.roll(u, 4, 0), 0.0)
        total = lane_roll(jnp.where(first_group, after, u), -32)
        total = total + lane_roll(jnp.where(last_group, prior, u), 32)
        total = total + lane_roll(jnp.where(not_first, u, 0.0), -1)
        total = total + lane_roll(jnp.where(not_last, u, 0.0), 1)
        if X > 0:
            total = total + fine[at, pl.ds(X * 32 - 32, 32), :]
        if X < 31:
            total = total + fine[at, pl.ds(X * 32 + 32, 32), :]
        return u, total

    def fine_sweeps(c):
        def sweep(s, carry):
            at = lax.rem(c + s, 2)
            for X in range(32):
                u, total = beside(at, X)
                rows = pl.ds(X * 32, 32)
                fine[1 - at, rows, :] = (1.0 - OMEGA) * u + fweight[rows, :] * (fsource[rows, :] + total)
            return carry

        lax.fori_loop(0, FSWEEPS, sweep, 0)

        at = lax.rem(c + FSWEEPS, 2)
        squares = jnp.zeros((8, 128), F32)
        for x in range(16):
            both = None
            for X in (2 * x, 2 * x + 1):
                u, total = beside(at, X)
                rows = pl.ds(X * 32, 32)
                rem = fsource[rows, :] - fdiag[rows, :] * u + total
                sq = rem * rem
                squares = squares + ((sq[0:8] + sq[8:16]) + (sq[16:24] + sq[24:32]))
                both = rem if both is None else both + rem
            for y2 in range(2):
                lo = both[8 * y2 : 8 * y2 + 8]
                hi = both[16 + 8 * y2 : 24 + 8 * y2]
                wide[pl.ds(8 * x, 8), pl.ds(256 * y2, 128)] = jnp.where(low4, lo, pltpu.roll(hi, 4, 0))
                wide[pl.ds(8 * x, 8), pl.ds(256 * y2 + 128, 128)] = jnp.where(
                    low4, pltpu.roll(lo, 4, 0), hi
                )
        live = (sub8 % 4).astype(F32) < count[...]
        fsum[c] = jnp.where(live, squares, 0.0)
        dense[...] = jnp.dot(
            wide[...], gather[...], precision=HIGHEST, preferred_element_type=F32
        )
        for j in range(SLOTS):
            for i in range(4):
                rblocks[j, pl.ds(8 * i, 8), :] = dense[pl.ds(32 * i + j, 8, stride=4), :]

    def send_restricted(c):
        def block_for(r, i):
            mark = code[r]
            value = rblocks[0, pl.ds(8 * i, 8), :]
            for j in range(1, SLOTS):
                value = jnp.where(mark == j, rblocks[j, pl.ds(8 * i, 8), :], value)
            return value

        for i in range(4):
            r_in[c, me, pl.ds(8 * i, 8), :] = block_for(me, i)

        def send(i, carry):
            q = lax.rem(me + members - i, members)
            for part in range(4):
                r_out[c, q, pl.ds(8 * part, 8), :] = block_for(q, part)
            pltpu.make_async_remote_copy(
                src_ref=r_out.at[c, q],
                dst_ref=r_in.at[c, me],
                send_sem=r_send.at[c],
                recv_sem=r_recv.at[c],
                device_id=peer(q),
                device_id_type=MESH,
            ).start()
            return carry

        lax.fori_loop(1, members, send, 0)

    def recv_restricted(c):
        wait_all(r_in.at[c], r_recv.at[c])
        blocks = [r_in[c, jnp.clip(o, 0, members - 1)] for o in owners]
        for p in range(16):
            value = zeros
            for s in range(SLOTS):
                value = jnp.where(places[s] == p, blocks[s], value)
            packed[p] = value
        for by in range(2):
            for i in range(4):
                parts = [packed[by * 8 + bz, pl.ds(8 * i, 8), :] for bz in range(8)]
                for k, part in enumerate(group_transpose(parts)):
                    mixed[pl.ds(k * 64 + by * 32 + 8 * i, 8), :] = part
        for x in range(16):
            for t in range(4):
                rows = pl.ds(x * 32 + 8 * t, 8)
                comp[rows, :] = (
                    source[rows, :]
                    + mixed[pl.ds(t // 2 * 32 + x * 2 + t % 2, 8, stride=64), :]
                )

    first_lane = lane32 == 0
    last_lane = lane32 == 127

    def coarse_sweep(c, k, last):
        halo(k, range(6), "recv")
        beyond = jnp.where(
            lane8 % 2 == 0,
            jnp.where(gz < n_z - 1, zhi[k], 0.0),
            jnp.where(gz > 0, zlo[k], 0.0),
        )
        acc = jnp.zeros((8, 128), F32)
        squares = jnp.zeros((8, 128), F32)
        for x in [0, 15] + list(range(1, 15)):
            rows = pl.ds(x * 32, 32)
            p = pot[k, rows, :]
            if x > 0:
                total = pot[k, pl.ds(x * 32 - 32, 32), :]
            else:
                total = jnp.where(gx > 0, xlo[k], 0.0)
            if x < 15:
                total = total + pot[k, pl.ds(x * 32 + 32, 32), :]
            else:
                total = total + jnp.where(gx < n_x - 1, xhi[k], 0.0)
            above = jnp.where(gy < n_y - 1, yhi[k, pl.ds(x, 1), :], 0.0)
            below = jnp.where(gy > 0, ylo[k, pl.ds(x, 1), :], 0.0)
            above = jnp.broadcast_to(above, (32, 128))
            below = jnp.broadcast_to(below, (32, 128))
            total = total + jnp.where(row32 == 31, above, pltpu.roll(p, 31, 0))
            total = total + jnp.where(row32 == 0, below, pltpu.roll(p, 1, 0))
            edge = jnp.concatenate(
                [lane_roll(beyond, -2 * (x * 4 + t)) for t in range(4)], axis=0
            )
            total = total + lane_roll(jnp.where(first_lane, edge, p), -1)
            total = total + lane_roll(jnp.where(last_lane, edge, p), 1)
            total = comp[rows, :] + total
            if last:
                res = total - diag[rows, :] * p
                sq = res * res
                squares = squares + ((sq[0:8] + sq[8:16]) + (sq[16:24] + sq[24:32]))
                new = p + weight[rows, :] * res
            else:
                new = (1.0 - OMEGA) * p + weight[rows, :] * total
            pot[k + 1, rows, :] = new
            acc = faces_of(x, new, k + 1, acc)
            if x == 15:
                halo(k + 1, (0, 1), "start")
        zface[k + 1] = acc
        halo(k + 1, (2, 3, 4, 5), "start")
        if last:
            csum[c] = squares

    loads[0].wait()
    acc = jnp.zeros((8, 128), F32)
    for x in range(16):
        acc = faces_of(x, pot[0, pl.ds(x * 32, 32), :], 0, acc)
    zface[0] = acc
    stage_surfaces()
    pl.semaphore_wait(barrier, members + 1)
    send_surfaces()
    halo(0, range(6), "start")

    rounds = []
    while 2 ** len(rounds) * 2 <= n_x // 2:
        rounds.append(2 ** len(rounds))

    def chain_step(at):
        if 0 < at <= len(rounds):
            pl.semaphore_wait(chain.at[at - 1], 2)
        if at < len(rounds):
            for way in (1, -1):
                pl.semaphore_signal(
                    chain.at[at],
                    inc=1,
                    device_id={"gx": ring(way * rounds[at])},
                    device_id_type=MESH,
                )

    chain_step(0)

    def prepare():
        i = lax.broadcasted_iota(jnp.int32, (128, 512), 0)
        n = lax.broadcasted_iota(jnp.int32, (128, 512), 1)
        lane = n % 128
        expand[...] = (i == (n // 128) * 32 + (lane // 64) * 16 + (lane % 32) // 2).astype(F32)
        n = lax.broadcasted_iota(jnp.int32, (512, 128), 0)
        o = lax.broadcasted_iota(jnp.int32, (512, 128), 1)
        lane = n % 128
        gather[...] = jnp.where(
            o == (n // 128) * 32 + (lane // 64) * 16 + (lane % 32) // 2, 0.125, 0.0
        )
        loads[2].wait()
        for x in range(16):
            rows = pl.ds(x * 32, 32)
            d = 6.0 + diag[rows, :]
            diag[rows, :] = d
            weight[rows, :] = OMEGA / d
        loads[4].wait()
        for X in range(32):
            rows = pl.ds(X * 32, 32)
            d = 6.0 + fdiag[rows, :]
            fdiag[rows, :] = d
            fweight[rows, :] = OMEGA / d
        for at in (1, 3, 5):
            loads[at].wait()

    norm_row = lax.broadcasted_iota(jnp.int32, (1, 128), 1)

    def norm_copy(src, dst, sem, device):
        return pltpu.make_async_remote_copy(
            src_ref=src,
            dst_ref=dst,
            send_sem=n_sem.at[sem],
            recv_sem=n_sem.at[sem + 1],
            device_id=device,
            device_id_type=MESH,
        )

    def send_norms():
        parts = [jnp.sum(csum[k] + fsum[k]) for k in range(CYCLES)]
        row = jnp.where(norm_row < 64, parts[0], parts[1])
        n_send[0] = row
        nx_in[gx] = row

        for i in sorted(range(1, n_x), key=lambda d: -min(d, n_x - d)):
            norm_copy(n_send.at[0], nx_in.at[gx], 0, {"gx": lax.rem(gx + i, n_x)}).start()

    def turn_norms():
        part = nx_in.at[pl.ds(0, n_x - 1)]
        pltpu.make_async_copy(part, part, n_sem.at[1]).wait()
        row = nx_in[0]
        for r in range(1, n_x):
            row = row + nx_in[r]
        n_send[1] = row
        np_in[me] = row

        def send(i, carry):
            norm_copy(n_send.at[1], np_in.at[me], 2, peer(lax.rem(me + i, members))).start()
            return carry

        lax.fori_loop(1, members, send, 0)

    def end_norms():
        wait_all(np_in, n_sem.at[3])
        row = np_in[0]
        for r in range(1, members):
            row = row + np_in[r]
        row = jnp.sqrt(row / cells)
        for k in range(CYCLES):
            norm_out[k] = row[0, 64 * k]

    def cycle(c, carry):
        use_parents(c)
        for k in range(CYCLES):

            @pl.when(c == k)
            def _(k=k):
                chain_step(2 * k + 1)

        fine_sweeps(c)
        send_restricted(c)
        for k in range(CYCLES):

            @pl.when(c == k)
            def _(k=k):
                chain_step(2 * k + 2)

        recv_restricted(c)

        def sweep(s, carry):
            coarse_sweep(c, c * CSWEEPS + s, False)
            return carry

        lax.fori_loop(0, CSWEEPS - 1, sweep, 0)
        coarse_sweep(c, c * CSWEEPS + CSWEEPS - 1, True)

        @pl.when(c == CYCLES - 1)
        def _():
            send_norms()

        send_parents(c)
        recv_parents(c)
        return carry

    prepare()
    recv_surfaces()
    lax.fori_loop(0, CYCLES, cycle, 0)

    pot_out[...] = pot[SWEEPS]
    live = ((row32 % 4).astype(F32) < jnp.concatenate([count[...]] * 4, axis=0)).astype(F32)
    end = CYCLES % 2
    for X in range(32):
        rows = pl.ds(X * 32, 32)
        fine_out[rows, :] = (fine[end, rows, :] + ghost[pl.ds(X // 2 * 32, 32), :]) * live
    turn_norms()

    wait_all(s_out, s_sem.at[0])
    for c in range(CYCLES):
        wait_all(d_out.at[c], d_send.at[c])
        wait_all(r_out.at[c], r_send.at[c])
    halo(SWEEPS, range(6), "recv")

    def left(k, carry):
        halo(k, range(6), "send")
        return carry

    lax.fori_loop(0, SWEEPS + 1, left, 0)
    part = nx_in.at[pl.ds(0, n_x - 1)]
    pltpu.make_async_copy(part, part, n_sem.at[0]).wait()
    end_norms()
    wait_all(np_in, n_sem.at[2])


def local(
    coarse_source,
    coarse_shift,
    coarse_start,
    fine_source,
    fine_shift,
    fine_start,
    box_corner,
    box_owner,
):
    n_x, n_y, n_z = (lax.axis_size(a) for a in ("gx", "gy", "gz"))
    members = n_y * n_z
    cells = float(n_x * n_y * n_z * coarse_source.size)

    def fine_rows(array):
        return array.reshape(SLOTS, 256, 128).transpose(1, 0, 2).reshape(FROWS, 128)

    hbm = pl.BlockSpec(memory_space=pltpu.HBM)
    smem = pl.BlockSpec(memory_space=pltpu.SMEM)
    vmem = pl.BlockSpec(memory_space=pltpu.VMEM)

    def buf(*shape):
        return pltpu.VMEM(shape, F32)

    sems = pltpu.SemaphoreType.DMA
    pot, fine, norms = pl.pallas_call(
        functools.partial(kernel, (n_x, n_y, n_z, cells)),
        out_shape=(
            jax.ShapeDtypeStruct((ROWS, 128), F32),
            jax.ShapeDtypeStruct((FROWS, 128), F32),
            jax.ShapeDtypeStruct((CYCLES,), F32),
        ),
        in_specs=[smem, smem] + [hbm] * 6,
        out_specs=(vmem, vmem, smem),
        scratch_shapes=[
            buf(SWEEPS + 1, ROWS, 128),
            buf(ROWS, 128),
            buf(ROWS, 128),
            buf(ROWS, 128),
            buf(ROWS, 128),
            buf(SWEEPS + 1, 32, 128),
            buf(SWEEPS + 1, 32, 128),
            buf(SWEEPS + 1, 16, 128),
            buf(SWEEPS + 1, 16, 128),
            buf(SWEEPS + 1, 8, 128),
            buf(SWEEPS + 1, 8, 128),
            buf(SWEEPS + 1, 2, 16, 128),
            buf(SWEEPS + 1, 8, 128),
            buf(2, FROWS, 128),
            buf(FROWS, 128),
            buf(FROWS, 128),
            buf(FROWS, 128),
            buf(128, 512),
            buf(512, 128),
            buf(128, 128),
            buf(ROWS, 128),
            buf(128, 512),
            buf(16, 32, 128),
            buf(ROWS, 128),
            buf(SLOTS, 32, 128),
            buf(members, 8, 128),
            buf(8, 128),
            pltpu.SMEM((members,), jnp.int32),
            pltpu.SMEM((members,), jnp.int32),
            pltpu.SMEM((members,), jnp.int32),
            buf(SLOTS, 12, 128),
            buf(members, 12, 128),
            buf(members, 12, 128),
            buf(CYCLES, members, 32, 128),
            buf(CYCLES, members, 32, 128),
            buf(CYCLES, members, 32, 128),
            buf(CYCLES, members, 32, 128),
            buf(CYCLES, 8, 128),
            buf(CYCLES, 8, 128),
            buf(n_x, 1, 128),
            buf(members, 1, 128),
            buf(2, 1, 128),
            sems((6,)),
            sems((2,)),
            sems((CYCLES,)),
            sems((CYCLES,)),
            sems((CYCLES,)),
            sems((CYCLES,)),
            sems((SWEEPS + 1, 6)),
            sems((SWEEPS + 1, 6)),
            sems((4,)),
            pltpu.SemaphoreType.REGULAR((4,)),
        ],
        compiler_params=pltpu.CompilerParams(
            collective_id=0, has_side_effects=True, vmem_limit_bytes=30 * 1000 * 1000
        ),
        name="cycles",
    )(
        box_corner.transpose(2, 0, 1),
        box_owner,
        *(
            pltpu.with_memory_space_constraint(array, pltpu.HBM)
            for array in (
                coarse_source.reshape(ROWS, 128),
                coarse_shift.reshape(ROWS, 128),
                coarse_start.reshape(ROWS, 128),
                fine_rows(fine_source),
                fine_rows(fine_shift),
                fine_rows(fine_start),
            )
        ),
    )
    fine = fine.reshape(256, SLOTS, 128).transpose(1, 0, 2).reshape(SLOTS, 256 * 128)
    return pot.reshape(coarse_source.shape), fine, norms


def solution(mesh):
    every = ("gx", "gy", "gz")
    return jax.shard_map(
        local,
        mesh=mesh,
        in_specs=(
            P("gx", "gy", "gz"),
            P("gx", "gy", "gz"),
            P("gx", "gy", "gz"),
            P(every, None),
            P(every, None),
            P(every, None),
            P(every, None, None),
            P(every, None),
        ),
        out_specs=(P("gx", "gy", "gz"), P(every, None), P()),
        check_vma=False,
    )
```

```python
import functools

import jax
import jax.numpy as jnp
from jax import lax
from jax.experimental import pallas as pl
from jax.experimental.pallas import tpu as pltpu
from jax.sharding import PartitionSpec as P

FOOT = 16
CYCLES = 2
CSWEEPS = 4
FSWEEPS = 3
SLOTS = 4
OMEGA = 0.8
HIGHEST = lax.Precision.HIGHEST
F32 = jnp.float32
MESH = pl.DeviceIdType.MESH

ROWS = 512
FROWS = 1024
SWEEPS = CYCLES * CSWEEPS
GATHERED = 4
PITCH = 72


def lane_roll(array, shift):
    return pltpu.roll(array, shift % 128, 1)


def group_transpose(parts):
    group = lax.broadcasted_iota(jnp.int32, (8, 128), 1) // 16
    parts = list(parts)
    for step in (1, 2, 4):
        clear = (group & step) == 0
        for i in range(8):
            if i & step:
                continue
            a, b = parts[i], parts[i + step]
            parts[i] = jnp.where(clear, a, lane_roll(b, 16 * step))
            parts[i + step] = jnp.where(clear, lane_roll(a, -16 * step), b)
    return parts


def kernel(
    sizes,
    corner,
    owner,
    source_hbm,
    shift_hbm,
    start_hbm,
    fsource_hbm,
    fshift_hbm,
    fstart_hbm,
    pot_out,
    fine_out,
    norm_out,
    pot,
    source,
    diag,
    weight,
    comp,
    beside_sum,
    xlo,
    xhi,
    ylo,
    yhi,
    zlo,
    zhi,
    yface,
    zface,
    fine,
    fsource,
    fdiag,
    fweight,
    expand,
    gather,
    dense,
    ghost,
    wide,
    packed,
    mixed,
    rblocks,
    code,
    count,
    place_of,
    slot_of,
    flag_of,
    surf,
    s_out,
    s_in,
    d_out,
    d_in,
    r_out,
    r_in,
    csum,
    fsum,
    nx_in,
    np_in,
    n_send,
    local_sem,
    s_sem,
    d_send,
    d_recv,
    r_send,
    r_recv,
    h_send,
    h_recv,
    n_sem,
    chain,
):
    n_x, n_y, n_z, cells = sizes
    members = n_y * n_z
    gx, gy, gz = lax.axis_index("gx"), lax.axis_index("gy"), lax.axis_index("gz")
    me = gy * n_z + gz

    def peer(q):
        return {"gy": q // n_z, "gz": lax.rem(q, n_z)}

    loads = [
        pltpu.make_async_copy(start_hbm, pot.at[0], local_sem.at[0]),
        pltpu.make_async_copy(source_hbm, source, local_sem.at[1]),
        pltpu.make_async_copy(shift_hbm, diag, local_sem.at[2]),
        pltpu.make_async_copy(fsource_hbm, fsource, local_sem.at[3]),
        pltpu.make_async_copy(fshift_hbm, fdiag, local_sem.at[4]),
        pltpu.make_async_copy(fstart_hbm, fine.at[0], local_sem.at[5]),
    ]
    for load in loads:
        load.start()

    barrier = pltpu.get_barrier_semaphore()

    def greet(i, carry):
        q = lax.rem(me + i, members)
        pl.semaphore_signal(barrier, inc=1, device_id=peer(q), device_id_type=MESH)
        return carry

    lax.fori_loop(1, members, greet, 0)

    def ring(distance):
        return lax.rem(gx + distance + n_x, n_x)

    for way in (1, -1):
        pl.semaphore_signal(barrier, inc=1, device_id={"gx": ring(way)}, device_id_type=MESH)

    owners = [owner[0, s] for s in range(SLOTS)]
    lives = [(o >= 0) & (o < members) for o in owners]
    places = [
        jnp.where(
            lives[s],
            ((corner[1, 0, s] >> 5) & 1) * 8 + ((corner[2, 0, s] >> 5) & 7),
            -1,
        )
        for s in range(SLOTS)
    ]
    for q in range(members):
        spot = jnp.int32(0)
        slot = jnp.int32(0)
        flag = jnp.int32(0)
        for s in range(SLOTS):
            mine = owners[s] == q
            spot = jnp.where(mine, places[s], spot)
            slot = jnp.where(mine, s, slot)
            flag = jnp.where(mine, 1, flag)
        place_of[q] = spot
        slot_of[q] = slot
        flag_of[q] = flag

    lane8 = lax.broadcasted_iota(jnp.int32, (8, 128), 1)
    sub8 = lax.broadcasted_iota(jnp.int32, (8, 128), 0)
    lane32 = lax.broadcasted_iota(jnp.int32, (32, 128), 1)
    row32 = lax.broadcasted_iota(jnp.int32, (32, 128), 0)
    low4 = sub8 < 4

    zeros = jnp.zeros((32, 128), F32)

    def halo(k, sides, act):
        routes = (
            (pot.at[k, pl.ds(0, 32)], xhi.at[k], {"gx": ring(-1)}),
            (pot.at[k, pl.ds(ROWS - 32, 32)], xlo.at[k], {"gx": ring(1)}),
            (yface.at[k, 0], yhi.at[k], {"gy": lax.rem(gy + n_y - 1, n_y)}),
            (yface.at[k, 1], ylo.at[k], {"gy": lax.rem(gy + 1, n_y)}),
            (zface.at[k], zhi.at[k], {"gz": lax.rem(gz + n_z - 1, n_z)}),
            (zface.at[k], zlo.at[k], {"gz": lax.rem(gz + 1, n_z)}),
        )
        for i in sides:
            src, dst, device = routes[i]
            copy = pltpu.make_async_remote_copy(
                src_ref=src,
                dst_ref=dst,
                send_sem=h_send.at[k, i],
                recv_sem=h_recv.at[k, i],
                device_id=device,
                device_id_type=MESH,
            )
            if act == "start":
                copy.start()
            elif act == "recv":
                copy.wait_recv()
            else:
                copy.wait_send()

    def faces_of(x, slab, k, acc):
        yface[k, 0, pl.ds(x, 1), :] = slab[0:1]
        yface[k, 1, pl.ds(x, 1), :] = slab[31:32]
        for t in range(4):
            v = x * 4 + t
            keep = (lane8 == 2 * v) | (lane8 == (2 * v - 1) % 128)
            acc = jnp.where(keep, lane_roll(slab[8 * t : 8 * t + 8], 2 * v), acc)
        return acc

    def pack_parents(slab_of):
        for x in range(16):
            slab = slab_of(x)
            for by in range(2):
                for y3 in range(2):
                    t = by * 2 + y3
                    mixed[pl.ds(by * 32 + x * 2 + y3, 8, stride=PITCH), :] = slab[8 * t : 8 * t + 8]
        for by in range(2):
            for i in range(4):
                parts = [mixed[pl.ds(k * PITCH + by * 32 + 8 * i, 8), :] for k in range(8)]
                for bz, part in enumerate(group_transpose(parts)):
                    packed[by * 8 + bz, pl.ds(8 * i, 8), :] = part

    def send_parents(c):
        rows_of = lambda at, x: pot[at, pl.ds(x * 32, 32), :]
        pack_parents(lambda x: rows_of(c * CSWEEPS + CSWEEPS, x) - rows_of(c * CSWEEPS, x))
        d_in[c, me] = packed[place_of[me]]

        def send(i, carry):
            q = lax.rem(me + members - i, members)
            d_out[c, q] = packed[place_of[q]]
            pltpu.make_async_remote_copy(
                src_ref=d_out.at[c, q],
                dst_ref=d_in.at[c, me],
                send_sem=d_send.at[c],
                recv_sem=d_recv.at[c],
                device_id=peer(q),
                device_id_type=MESH,
            ).start()
            return carry

        lax.fori_loop(1, members, send, 0)

    inner_lane = lambda lane, first: (lane > first) & (lane < first + 15)

    def surface_lane(o):
        m = o % 32
        at = jnp.where(m < 16, m, ((m - 16) // 2 + 1) * 16 + (m % 2) * 15)
        return jnp.where(m < 30, at, -1)

    def stage_surfaces():
        pack_parents(lambda x: pot[0, pl.ds(x * 32, 32), :])
        i = lax.broadcasted_iota(jnp.int32, (128, 128), 0)
        o = lax.broadcasted_iota(jnp.int32, (128, 128), 1)
        choose = (i == surface_lane(o)).astype(F32)
        for s in range(SLOTS):
            block = packed[jnp.maximum(places[s], 0)]
            odd = (row32 % 2 == 1) & inner_lane(lane32, 0)
            dense[pl.ds(32 * s, 32), :] = jnp.where(odd, lane_roll(block, 16), block)
            surf[s, pl.ds(8, 2), :] = block[0:2]
            surf[s, pl.ds(10, 2), :] = block[30:32]
        ghost[pl.ds(0, 128), :] = jnp.dot(
            dense[...], choose, precision=HIGHEST, preferred_element_type=F32
        )
        for s in range(SLOTS):
            block = ghost[pl.ds(32 * s, 32), :]
            block = jnp.where(lane32 // 32 == row32 % 4, block, 0.0)
            block = block + pltpu.roll(block, 31, 0)
            block = block + pltpu.roll(block, 30, 0)
            dense[pl.ds(32 * s, 32), :] = block
            surf[s, pl.ds(0, 8), :] = dense[pl.ds(32 * s, 8, stride=4), :]

        def stage(q, carry):
            slot = slot_of[q]
            flag = jnp.full((8, 128), flag_of[q].astype(F32), F32)
            s_out[q, pl.ds(0, 8), :] = jnp.where(lane8 == 31, flag, surf[slot, pl.ds(0, 8), :])
            s_out[q, pl.ds(8, 4), :] = surf[slot, pl.ds(8, 4), :]
            return carry

        lax.fori_loop(0, members, stage, 0)
        s_in[me] = s_out[me]

    def send_surfaces():
        def send(i, carry):
            q = lax.rem(me + members - i, members)
            pltpu.make_async_remote_copy(
                src_ref=s_out.at[q],
                dst_ref=s_in.at[me],
                send_sem=s_sem.at[0],
                recv_sem=s_sem.at[1],
                device_id=peer(q),
                device_id_type=MESH,
            ).start()
            return carry

        lax.fori_loop(1, members, send, 0)

    def recv_surfaces():
        wait_all(s_in, s_sem.at[1])
        before = jnp.zeros((8, 128), F32)
        tops = [jnp.zeros((8, 128), F32)] * SLOTS
        ends = [jnp.zeros((4, 128), F32)] * SLOTS
        for r in range(members):
            top = s_in[r, pl.ds(0, 8), :]
            end = s_in[r, pl.ds(8, 4), :]
            flag = jnp.sum(jnp.where(lane8 == 31, top, 0.0), axis=1, keepdims=True)
            flag = jnp.broadcast_to(flag, (8, 128))
            mark = jnp.where(flag > 0.5, before, -1.0)
            code[r] = mark
            before = before + flag
            for j in range(SLOTS):
                tops[j] = jnp.where(mark == j, top, tops[j])
                ends[j] = jnp.where(mark[0:4] == j, end, ends[j])
        count[...] = before
        for j in range(SLOTS):
            for i in range(4):
                dense[pl.ds(4 * i + j, 8, stride=16), :] = jnp.where(
                    lane8 // 32 == i, tops[j], 0.0
                )
        i = lax.broadcasted_iota(jnp.int32, (128, 128), 0)
        o = lax.broadcasted_iota(jnp.int32, (128, 128), 1)
        place = (surface_lane(i) == o).astype(F32)
        value = jnp.dot(dense[...], place, precision=HIGHEST, preferred_element_type=F32)
        odd = ((i // 4) % 2 == 1) & inner_lane(o, 112)
        dense[...] = jnp.where(odd, lane_roll(value, 112), value)
        for j in range(SLOTS):
            for y3 in range(2):
                dense[pl.ds(y3 * 4 + j, 1), :] = ends[j][y3 : y3 + 1]
                dense[pl.ds(120 + y3 * 4 + j, 1), :] = ends[j][2 + y3 : 3 + y3]
        spread()

    def wait_all(buffer, sem):
        part = buffer.at[pl.ds(0, members - 1)]
        pltpu.make_async_copy(part, part, sem).wait()

    def recv_parents(c):
        wait_all(d_in.at[c], d_recv.at[c])

        def pick(r8, acc):
            acc = list(acc)
            for r in range(GATHERED):
                r = r8 * GATHERED + r
                mark = code[r]
                for i in range(4):
                    data = d_in[c, r, pl.ds(8 * i, 8), :]
                    for j in range(SLOTS):
                        acc[j * 4 + i] = jnp.where(mark == j, data, acc[j * 4 + i])
            return tuple(acc)

        blank = jnp.zeros((8, 128), F32)
        acc = lax.fori_loop(0, members // GATHERED, pick, (blank,) * 16)
        for j in range(SLOTS):
            for i in range(4):
                dense[pl.ds(32 * i + j, 8, stride=4), :] = acc[j * 4 + i]
        spread()

    def spread():
        for y2 in range(2):
            a = jnp.dot(
                dense[...], expand[:, pl.ds(256 * y2, 128)], precision=HIGHEST,
                preferred_element_type=F32,
            )
            b = jnp.dot(
                dense[...], expand[:, pl.ds(256 * y2 + 128, 128)], precision=HIGHEST,
                preferred_element_type=F32,
            )
            for x in range(16):
                ax, bx = a[8 * x : 8 * x + 8], b[8 * x : 8 * x + 8]
                ghost[pl.ds(x * 32 + y2 * 8, 8), :] = jnp.where(low4, ax, pltpu.roll(bx, 4, 0))
                ghost[pl.ds(x * 32 + 16 + y2 * 8, 8), :] = jnp.where(low4, pltpu.roll(ax, 4, 0), bx)

    fine_y = (row32 // 4) * 4 + lane32 // 32
    fine_z = lane32 % 32
    sides = (
        (fine_y == 0).astype(F32)
        + (fine_y == 31).astype(F32)
        + (fine_z == 0).astype(F32)
        + (fine_z == 31).astype(F32)
    )

    def use_parents(c):
        for X in range(32):
            g = ghost[pl.ds(X // 2 * 32, 32), :]
            times = sides + 1.0 if X in (0, 31) else sides
            fsource[pl.ds(X * 32, 32), :] = fsource[pl.ds(X * 32, 32), :] + times * g

        @pl.when(c > 0)
        def _():
            for X in range(32):
                at = lax.rem(c, 2)
                fine[at, pl.ds(X * 32, 32), :] = (
                    fine[at, pl.ds(X * 32, 32), :] + ghost[pl.ds(X // 2 * 32, 32), :]
                )

    not_first = fine_z > 0
    not_last = fine_z < 31
    first_group = lane32 < 32
    last_group = lane32 >= 96

    def beside(at, X):
        u = fine[at, pl.ds(X * 32, 32), :]
        after = jnp.where(row32 < 28, pltpu.roll(u, 28, 0), 0.0)
        prior = jnp.where(row32 >= 4, pltpu.roll(u, 4, 0), 0.0)
        total = lane_roll(jnp.where(first_group, after, u), -32)
        total = total + lane_roll(jnp.where(last_group, prior, u), 32)
        total = total + lane_roll(jnp.where(not_first, u, 0.0), -1)
        total = total + lane_roll(jnp.where(not_last, u, 0.0), 1)
        if X > 0:
            total = total + fine[at, pl.ds(X * 32 - 32, 32), :]
        if X < 31:
            total = total + fine[at, pl.ds(X * 32 + 32, 32), :]
        return u, total

    def fine_sweeps(c):
        def sweep(s, carry):
            at = lax.rem(c + s, 2)
            for X in range(32):
                u, total = beside(at, X)
                rows = pl.ds(X * 32, 32)
                fine[1 - at, rows, :] = (1.0 - OMEGA) * u + fweight[rows, :] * (fsource[rows, :] + total)
            return carry

        lax.fori_loop(0, FSWEEPS, sweep, 0)

        at = lax.rem(c + FSWEEPS, 2)
        squares = jnp.zeros((8, 128), F32)
        for x in range(16):
            both = None
            for X in (2 * x, 2 * x + 1):
                u, total = beside(at, X)
                rows = pl.ds(X * 32, 32)
                rem = fsource[rows, :] - fdiag[rows, :] * u + total
                sq = rem * rem
                squares = squares + ((sq[0:8] + sq[8:16]) + (sq[16:24] + sq[24:32]))
                both = rem if both is None else both + rem
            for y2 in range(2):
                lo = both[8 * y2 : 8 * y2 + 8]
                hi = both[16 + 8 * y2 : 24 + 8 * y2]
                wide[pl.ds(8 * x, 8), pl.ds(256 * y2, 128)] = jnp.where(low4, lo, pltpu.roll(hi, 4, 0))
                wide[pl.ds(8 * x, 8), pl.ds(256 * y2 + 128, 128)] = jnp.where(
                    low4, pltpu.roll(lo, 4, 0), hi
                )
        live = (sub8 % 4).astype(F32) < count[...]
        fsum[c] = jnp.where(live, squares, 0.0)
        dense[...] = jnp.dot(
            wide[...], gather[...], precision=HIGHEST, preferred_element_type=F32
        )
        for j in range(SLOTS):
            for i in range(4):
                rblocks[j, pl.ds(8 * i, 8), :] = dense[pl.ds(32 * i + j, 8, stride=4), :]

    def send_restricted(c):
        def block_for(r, i):
            mark = code[r]
            value = rblocks[0, pl.ds(8 * i, 8), :]
            for j in range(1, SLOTS):
                value = jnp.where(mark == j, rblocks[j, pl.ds(8 * i, 8), :], value)
            return value

        for i in range(4):
            r_in[c, me, pl.ds(8 * i, 8), :] = block_for(me, i)

        def send(i, carry):
            q = lax.rem(me + members - i, members)
            for part in range(4):
                r_out[c, q, pl.ds(8 * part, 8), :] = block_for(q, part)
            pltpu.make_async_remote_copy(
                src_ref=r_out.at[c, q],
                dst_ref=r_in.at[c, me],
                send_sem=r_send.at[c],
                recv_sem=r_recv.at[c],
                device_id=peer(q),
                device_id_type=MESH,
            ).start()
            return carry

        lax.fori_loop(1, members, send, 0)

    def recv_restricted(c):
        wait_all(r_in.at[c], r_recv.at[c])
        blocks = [r_in[c, jnp.clip(o, 0, members - 1)] for o in owners]
        for p in range(16):
            value = zeros
            for s in range(SLOTS):
                value = jnp.where(places[s] == p, blocks[s], value)
            packed[p] = value
        for by in range(2):
            for i in range(4):
                parts = [packed[by * 8 + bz, pl.ds(8 * i, 8), :] for bz in range(8)]
                for k, part in enumerate(group_transpose(parts)):
                    mixed[pl.ds(k * PITCH + by * 32 + 8 * i, 8), :] = part
        for x in range(16):
            for t in range(4):
                rows = pl.ds(x * 32 + 8 * t, 8)
                comp[rows, :] = (
                    source[rows, :]
                    + mixed[pl.ds(t // 2 * 32 + x * 2 + t % 2, 8, stride=PITCH), :]
                )

    edge_lane = (lane8 == 0) | (lane8 == 127)

    def coarse_inner(k):
        for x in range(16):
            p = pot[k, pl.ds(x * 32, 32), :]
            total = jnp.where(row32 < 31, pltpu.roll(p, 31, 0), 0.0)
            total = total + jnp.where(row32 > 0, pltpu.roll(p, 1, 0), 0.0)
            total = total + jnp.where(lane32 < 127, lane_roll(p, -1), 0.0)
            total = total + jnp.where(lane32 > 0, lane_roll(p, 1), 0.0)
            if x > 0:
                total = total + pot[k, pl.ds(x * 32 - 32, 32), :]
            if x < 15:
                total = total + pot[k, pl.ds(x * 32 + 32, 32), :]
            beside_sum[pl.ds(x * 32, 32), :] = total

    def coarse_sweep(c, k, last):
        halo(k, range(6), "recv")
        beyond = jnp.where(
            lane8 % 2 == 0,
            jnp.where(gz > 0, lane_roll(zlo[k], 1), 0.0),
            jnp.where(gz < n_z - 1, lane_roll(zhi[k], -1), 0.0),
        )
        acc = jnp.zeros((8, 128), F32)
        squares = jnp.zeros((8, 128), F32)
        for x in [0, 15] + list(range(1, 15)):
            rows = pl.ds(x * 32, 32)
            p = pot[k, rows, :]
            total = comp[rows, :] + beside_sum[rows, :]
            if x == 0:
                total = total + jnp.where(gx > 0, xlo[k], 0.0)
            if x == 15:
                total = total + jnp.where(gx < n_x - 1, xhi[k], 0.0)
            above = jnp.where(gy < n_y - 1, yhi[k, pl.ds(x, 1), :], 0.0)
            below = jnp.where(gy > 0, ylo[k, pl.ds(x, 1), :], 0.0)
            parts = []
            for t in range(4):
                edge = lane_roll(beyond, -2 * (x * 4 + t))
                part = total[8 * t : 8 * t + 8] + jnp.where(edge_lane, edge, 0.0)
                if t == 0:
                    part = part + jnp.where(sub8 == 0, jnp.broadcast_to(below, (8, 128)), 0.0)
                if t == 3:
                    part = part + jnp.where(sub8 == 7, jnp.broadcast_to(above, (8, 128)), 0.0)
                parts.append(part)
            total = jnp.concatenate(parts, axis=0)
            if last:
                res = total - diag[rows, :] * p
                sq = res * res
                squares = squares + ((sq[0:8] + sq[8:16]) + (sq[16:24] + sq[24:32]))
                new = p + weight[rows, :] * res
            else:
                new = (1.0 - OMEGA) * p + weight[rows, :] * total
            pot[k + 1, rows, :] = new
            acc = faces_of(x, new, k + 1, acc)
            if x == 15:
                halo(k + 1, (0, 1), "start")
        zface[k + 1] = acc
        halo(k + 1, (2, 3, 4, 5), "start")
        if last:
            csum[c] = squares

    loads[0].wait()
    acc = jnp.zeros((8, 128), F32)
    for x in range(16):
        acc = faces_of(x, pot[0, pl.ds(x * 32, 32), :], 0, acc)
    zface[0] = acc
    stage_surfaces()
    pl.semaphore_wait(barrier, members + 1)
    send_surfaces()
    halo(0, range(6), "start")

    rounds = []
    while 2 ** len(rounds) * 2 <= n_x // 2:
        rounds.append(2 ** len(rounds))

    def chain_step(at):
        if 0 < at <= len(rounds):
            pl.semaphore_wait(chain.at[at - 1], 2)
        if at < len(rounds):
            for way in (1, -1):
                pl.semaphore_signal(
                    chain.at[at],
                    inc=1,
                    device_id={"gx": ring(way * rounds[at])},
                    device_id_type=MESH,
                )

    chain_step(0)

    def prepare():
        i = lax.broadcasted_iota(jnp.int32, (128, 512), 0)
        n = lax.broadcasted_iota(jnp.int32, (128, 512), 1)
        lane = n % 128
        expand[...] = (i == (n // 128) * 32 + (lane // 64) * 16 + (lane % 32) // 2).astype(F32)
        n = lax.broadcasted_iota(jnp.int32, (512, 128), 0)
        o = lax.broadcasted_iota(jnp.int32, (512, 128), 1)
        lane = n % 128
        gather[...] = jnp.where(
            o == (n // 128) * 32 + (lane // 64) * 16 + (lane % 32) // 2, 0.125, 0.0
        )
        loads[2].wait()
        for x in range(16):
            rows = pl.ds(x * 32, 32)
            d = 6.0 + diag[rows, :]
            diag[rows, :] = d
            weight[rows, :] = OMEGA / d
        loads[4].wait()
        for X in range(32):
            rows = pl.ds(X * 32, 32)
            d = 6.0 + fdiag[rows, :]
            fdiag[rows, :] = d
            fweight[rows, :] = OMEGA / d
        for at in (1, 3, 5):
            loads[at].wait()

    norm_row = lax.broadcasted_iota(jnp.int32, (1, 128), 1)

    def norm_copy(src, dst, sem, device):
        return pltpu.make_async_remote_copy(
            src_ref=src,
            dst_ref=dst,
            send_sem=n_sem.at[sem],
            recv_sem=n_sem.at[sem + 1],
            device_id=device,
            device_id_type=MESH,
        )

    def send_norms():
        parts = [jnp.sum(csum[k] + fsum[k]) for k in range(CYCLES)]
        row = jnp.where(norm_row < 64, parts[0], parts[1])
        n_send[0] = row
        nx_in[gx] = row

        for i in sorted(range(1, n_x), key=lambda d: -min(d, n_x - d)):
            norm_copy(n_send.at[0], nx_in.at[gx], 0, {"gx": lax.rem(gx + i, n_x)}).start()

    def turn_norms():
        part = nx_in.at[pl.ds(0, n_x - 1)]
        pltpu.make_async_copy(part, part, n_sem.at[1]).wait()
        row = nx_in[0]
        for r in range(1, n_x):
            row = row + nx_in[r]
        n_send[1] = row
        np_in[me] = row

        def send(i, carry):
            norm_copy(n_send.at[1], np_in.at[me], 2, peer(lax.rem(me + i, members))).start()
            return carry

        lax.fori_loop(1, members, send, 0)

    def end_norms():
        wait_all(np_in, n_sem.at[3])
        row = np_in[0]
        for r in range(1, members):
            row = row + np_in[r]
        row = jnp.sqrt(row / cells)
        for k in range(CYCLES):
            norm_out[k] = row[0, 64 * k]

    def cycle(c, carry):
        use_parents(c)
        for k in range(CYCLES):

            @pl.when(c == k)
            def _(k=k):
                chain_step(2 * k + 1)

        fine_sweeps(c)
        send_restricted(c)
        for k in range(CYCLES):

            @pl.when(c == k)
            def _(k=k):
                chain_step(2 * k + 2)

        recv_restricted(c)

        def sweep(s, carry):
            coarse_sweep(c, c * CSWEEPS + s, False)
            coarse_inner(c * CSWEEPS + s + 1)
            return carry

        lax.fori_loop(0, CSWEEPS - 1, sweep, 0)
        coarse_sweep(c, c * CSWEEPS + CSWEEPS - 1, True)

        @pl.when(c == CYCLES - 1)
        def _():
            send_norms()

        send_parents(c)
        coarse_inner(c * CSWEEPS + CSWEEPS)
        recv_parents(c)
        return carry

    prepare()
    coarse_inner(0)
    recv_surfaces()
    lax.fori_loop(0, CYCLES, cycle, 0)

    pot_out[...] = pot[SWEEPS]
    live = ((row32 % 4).astype(F32) < jnp.concatenate([count[...]] * 4, axis=0)).astype(F32)
    end = CYCLES % 2
    for X in range(32):
        rows = pl.ds(X * 32, 32)
        fine_out[rows, :] = (fine[end, rows, :] + ghost[pl.ds(X // 2 * 32, 32), :]) * live
    turn_norms()

    wait_all(s_out, s_sem.at[0])
    for c in range(CYCLES):
        wait_all(d_out.at[c], d_send.at[c])
        wait_all(r_out.at[c], r_send.at[c])
    halo(SWEEPS, range(6), "recv")

    def left(k, carry):
        halo(k, range(6), "send")
        return carry

    lax.fori_loop(0, SWEEPS + 1, left, 0)
    part = nx_in.at[pl.ds(0, n_x - 1)]
    pltpu.make_async_copy(part, part, n_sem.at[0]).wait()
    end_norms()
    wait_all(np_in, n_sem.at[2])


def local(
    coarse_source,
    coarse_shift,
    coarse_start,
    fine_source,
    fine_shift,
    fine_start,
    box_corner,
    box_owner,
):
    n_x, n_y, n_z = (lax.axis_size(a) for a in ("gx", "gy", "gz"))
    members = n_y * n_z
    cells = float(n_x * n_y * n_z * coarse_source.size)

    def fine_rows(array):
        return array.reshape(SLOTS, 256, 128).transpose(1, 0, 2).reshape(FROWS, 128)

    hbm = pl.BlockSpec(memory_space=pltpu.HBM)
    smem = pl.BlockSpec(memory_space=pltpu.SMEM)
    vmem = pl.BlockSpec(memory_space=pltpu.VMEM)

    def buf(*shape):
        return pltpu.VMEM(shape, F32)

    sems = pltpu.SemaphoreType.DMA
    pot, fine, norms = pl.pallas_call(
        functools.partial(kernel, (n_x, n_y, n_z, cells)),
        out_shape=(
            jax.ShapeDtypeStruct((ROWS, 128), F32),
            jax.ShapeDtypeStruct((FROWS, 128), F32),
            jax.ShapeDtypeStruct((CYCLES,), F32),
        ),
        in_specs=[smem, smem] + [hbm] * 6,
        out_specs=(vmem, vmem, smem),
        scratch_shapes=[
            buf(SWEEPS + 1, ROWS, 128),
            buf(ROWS, 128),
            buf(ROWS, 128),
            buf(ROWS, 128),
            buf(ROWS, 128),
            buf(ROWS, 128),
            buf(SWEEPS + 1, 32, 128),
            buf(SWEEPS + 1, 32, 128),
            buf(SWEEPS + 1, 16, 128),
            buf(SWEEPS + 1, 16, 128),
            buf(SWEEPS + 1, 8, 128),
            buf(SWEEPS + 1, 8, 128),
            buf(SWEEPS + 1, 2, 16, 128),
            buf(SWEEPS + 1, 8, 128),
            buf(2, FROWS, 128),
            buf(FROWS, 128),
            buf(FROWS, 128),
            buf(FROWS, 128),
            buf(128, 512),
            buf(512, 128),
            buf(128, 128),
            buf(ROWS, 128),
            buf(128, 512),
            buf(16, 32, 128),
            buf(8 * PITCH, 128),
            buf(SLOTS, 32, 128),
            buf(members, 8, 128),
            buf(8, 128),
            pltpu.SMEM((members,), jnp.int32),
            pltpu.SMEM((members,), jnp.int32),
            pltpu.SMEM((members,), jnp.int32),
            buf(SLOTS, 12, 128),
            buf(members, 12, 128),
            buf(members, 12, 128),
            buf(CYCLES, members, 32, 128),
            buf(CYCLES, members, 32, 128),
            buf(CYCLES, members, 32, 128),
            buf(CYCLES, members, 32, 128),
            buf(CYCLES, 8, 128),
            buf(CYCLES, 8, 128),
            buf(n_x, 1, 128),
            buf(members, 1, 128),
            buf(2, 1, 128),
            sems((6,)),
            sems((2,)),
            sems((CYCLES,)),
            sems((CYCLES,)),
            sems((CYCLES,)),
            sems((CYCLES,)),
            sems((SWEEPS + 1, 6)),
            sems((SWEEPS + 1, 6)),
            sems((4,)),
            pltpu.SemaphoreType.REGULAR((4,)),
        ],
        compiler_params=pltpu.CompilerParams(
            collective_id=0, has_side_effects=True, vmem_limit_bytes=30 * 1000 * 1000
        ),
        name="cycles",
    )(
        box_corner.transpose(2, 0, 1),
        box_owner,
        *(
            pltpu.with_memory_space_constraint(array, pltpu.HBM)
            for array in (
                coarse_source.reshape(ROWS, 128),
                coarse_shift.reshape(ROWS, 128),
                coarse_start.reshape(ROWS, 128),
                fine_rows(fine_source),
                fine_rows(fine_shift),
                fine_rows(fine_start),
            )
        ),
    )
    fine = fine.reshape(256, SLOTS, 128).transpose(1, 0, 2).reshape(SLOTS, 256 * 128)
    return pot.reshape(coarse_source.shape), fine, norms


def solution(mesh):
    every = ("gx", "gy", "gz")
    return jax.shard_map(
        local,
        mesh=mesh,
        in_specs=(
            P("gx", "gy", "gz"),
            P("gx", "gy", "gz"),
            P("gx", "gy", "gz"),
            P(every, None),
            P(every, None),
            P(every, None),
            P(every, None, None),
            P(every, None),
        ),
        out_specs=(P("gx", "gy", "gz"), P(every, None), P()),
        check_vma=False,
    )
```

```python
import functools

import jax
import jax.numpy as jnp
from jax import lax
from jax.experimental import pallas as pl
from jax.experimental.pallas import tpu as pltpu
from jax.sharding import PartitionSpec as P

FOOT = 16
CYCLES = 2
CSWEEPS = 4
FSWEEPS = 3
SLOTS = 4
OMEGA = 0.8
HIGHEST = lax.Precision.HIGHEST
F32 = jnp.float32
MESH = pl.DeviceIdType.MESH

ROWS = 512
FROWS = 1024
SWEEPS = CYCLES * CSWEEPS
GATHERED = 4
PITCH = 72


def lane_roll(array, shift):
    return pltpu.roll(array, shift % 128, 1)


def in_parts(value):
    parts = []
    for _ in range(3):
        cut = value.astype(jnp.bfloat16)
        parts.append(cut)
        value = value - cut.astype(F32)
    return parts


def kernel(
    sizes,
    corner_hbm,
    owner_hbm,
    source_hbm,
    shift_hbm,
    start_hbm,
    fsource_hbm,
    fshift_hbm,
    fstart_hbm,
    pot_out,
    fine_out,
    norm_out,
    pot,
    source,
    diag,
    weight,
    comp,
    beside_sum,
    xlo,
    xhi,
    ylo,
    yhi,
    zlo,
    zhi,
    yface,
    zface,
    fine,
    fsource,
    fdiag,
    fweight,
    expand,
    gather,
    dense,
    ghost,
    wide,
    packed,
    halves,
    placed,
    lane_in,
    lane_out,
    mixed,
    rblocks,
    code,
    count,
    corner,
    owner,
    slot_of,
    flag_of,
    surf,
    s_out,
    s_in,
    d_out,
    d_in,
    r_out,
    r_in,
    csum,
    fsum,
    nx_in,
    np_in,
    n_send,
    local_sem,
    s_sem,
    d_send,
    d_recv,
    r_send,
    r_recv,
    h_send,
    h_recv,
    n_sem,
    chain,
):
    n_x, n_y, n_z, cells = sizes
    members = n_y * n_z
    gx, gy, gz = lax.axis_index("gx"), lax.axis_index("gy"), lax.axis_index("gz")
    me = gy * n_z + gz

    def peer(q):
        return {"gy": q // n_z, "gz": lax.rem(q, n_z)}

    barrier = pltpu.get_barrier_semaphore()

    def greet(i, carry):
        q = lax.rem(me + i, members)
        pl.semaphore_signal(barrier, inc=1, device_id=peer(q), device_id_type=MESH)
        return carry

    lax.fori_loop(1, members, greet, 0)

    def ring(distance):
        return lax.rem(gx + distance + n_x, n_x)

    for way in (1, -1):
        pl.semaphore_signal(barrier, inc=1, device_id={"gx": ring(way)}, device_id_type=MESH)

    tables = [
        pltpu.make_async_copy(corner_hbm, corner, local_sem.at[6]),
        pltpu.make_async_copy(owner_hbm, owner, local_sem.at[7]),
    ]
    loads = [
        pltpu.make_async_copy(start_hbm, pot.at[0], local_sem.at[0]),
        pltpu.make_async_copy(source_hbm, source, local_sem.at[1]),
        pltpu.make_async_copy(shift_hbm, diag, local_sem.at[2]),
        pltpu.make_async_copy(fsource_hbm, fsource, local_sem.at[3]),
        pltpu.make_async_copy(fshift_hbm, fdiag, local_sem.at[4]),
        pltpu.make_async_copy(fstart_hbm, fine.at[0], local_sem.at[5]),
    ]
    for load in tables + loads:
        load.start()

    for table in tables:
        table.wait()
    owners = [owner[0, s] for s in range(SLOTS)]
    lives = [(o >= 0) & (o < members) for o in owners]
    places = [
        jnp.where(
            lives[s],
            ((corner[1, 0, s] >> 5) & 1) * 8 + ((corner[2, 0, s] >> 5) & 7),
            -1,
        )
        for s in range(SLOTS)
    ]
    spots = [jnp.maximum(place, 0) for place in places]
    for q in range(members):
        slot = jnp.int32(0)
        flag = jnp.int32(0)
        for s in range(SLOTS):
            mine = owners[s] == q
            slot = jnp.where(mine, s, slot)
            flag = jnp.where(mine, 1, flag)
        slot_of[q] = slot
        flag_of[q] = flag
    i = lax.broadcasted_iota(jnp.int32, (384, 128), 0) % 128
    o = lax.broadcasted_iota(jnp.int32, (384, 128), 1)
    for s in range(SLOTS):
        group = spots[s] & 7
        lane_in[s] = ((i % 16 == o % 16) & (i // 16 == group)).astype(F32).astype(jnp.bfloat16)
        lane_out[s] = ((i % 16 == o % 16) & (o // 16 == group)).astype(F32).astype(jnp.bfloat16)

    lane8 = lax.broadcasted_iota(jnp.int32, (8, 128), 1)
    sub8 = lax.broadcasted_iota(jnp.int32, (8, 128), 0)
    lane32 = lax.broadcasted_iota(jnp.int32, (32, 128), 1)
    row32 = lax.broadcasted_iota(jnp.int32, (32, 128), 0)
    low4 = sub8 < 4

    zeros = jnp.zeros((32, 128), F32)

    def halo(k, sides, act):
        routes = (
            (pot.at[k, pl.ds(0, 32)], xhi.at[k], {"gx": ring(-1)}),
            (pot.at[k, pl.ds(ROWS - 32, 32)], xlo.at[k], {"gx": ring(1)}),
            (yface.at[k, 0], yhi.at[k], {"gy": lax.rem(gy + n_y - 1, n_y)}),
            (yface.at[k, 1], ylo.at[k], {"gy": lax.rem(gy + 1, n_y)}),
            (zface.at[k], zhi.at[k], {"gz": lax.rem(gz + n_z - 1, n_z)}),
            (zface.at[k], zlo.at[k], {"gz": lax.rem(gz + 1, n_z)}),
        )
        for i in sides:
            src, dst, device = routes[i]
            copy = pltpu.make_async_remote_copy(
                src_ref=src,
                dst_ref=dst,
                send_sem=h_send.at[k, i],
                recv_sem=h_recv.at[k, i],
                device_id=device,
                device_id_type=MESH,
            )
            if act == "start":
                copy.start()
            elif act == "recv":
                copy.wait_recv()
            else:
                copy.wait_send()

    def faces_of(x, slab, k, acc):
        yface[k, 0, pl.ds(x, 1), :] = slab[0:1]
        yface[k, 1, pl.ds(x, 1), :] = slab[31:32]
        for t in range(4):
            v = x * 4 + t
            keep = (lane8 == 2 * v) | (lane8 == (2 * v - 1) % 128)
            acc = jnp.where(keep, lane_roll(slab[8 * t : 8 * t + 8], 2 * v), acc)
        return acc

    def pack_parents(slab_of):
        for x in range(16):
            slab = slab_of(x)
            for by in range(2):
                for y3 in range(2):
                    t = by * 2 + y3
                    mixed[pl.ds(by * 32 + x * 2 + y3, 8, stride=PITCH), :] = slab[8 * t : 8 * t + 8]
        for by in range(2):
            for k in range(8):
                value = mixed[pl.ds(k * PITCH + by * 32, 32), :]
                for p, part in enumerate(in_parts(value)):
                    halves[by, pl.ds(k * 32, 32), pl.ds(128 * p, 128)] = part
        for s in range(SLOTS):
            rows = jnp.dot(
                halves[spots[s] >> 3], lane_in[s], preferred_element_type=F32
            )
            value = rows[0:32]
            for k in range(1, 8):
                value = jnp.where(lane32 // 16 == k, rows[32 * k : 32 * k + 32], value)
            packed[s] = value

    def send_parents(c):
        rows_of = lambda at, x: pot[at, pl.ds(x * 32, 32), :]
        pack_parents(lambda x: rows_of(c * CSWEEPS + CSWEEPS, x) - rows_of(c * CSWEEPS, x))
        d_in[c, me] = packed[slot_of[me]]

        def send(i, carry):
            q = lax.rem(me + members - i, members)
            d_out[c, q] = packed[slot_of[q]]
            pltpu.make_async_remote_copy(
                src_ref=d_out.at[c, q],
                dst_ref=d_in.at[c, me],
                send_sem=d_send.at[c],
                recv_sem=d_recv.at[c],
                device_id=peer(q),
                device_id_type=MESH,
            ).start()
            return carry

        lax.fori_loop(1, members, send, 0)

    inner_lane = lambda lane, first: (lane > first) & (lane < first + 15)

    def surface_lane(o):
        m = o % 32
        at = jnp.where(m < 16, m, ((m - 16) // 2 + 1) * 16 + (m % 2) * 15)
        return jnp.where(m < 30, at, -1)

    def stage_surfaces():
        pack_parents(lambda x: pot[0, pl.ds(x * 32, 32), :])
        i = lax.broadcasted_iota(jnp.int32, (128, 128), 0)
        o = lax.broadcasted_iota(jnp.int32, (128, 128), 1)
        choose = (i == surface_lane(o)).astype(F32)
        for s in range(SLOTS):
            block = packed[s]
            odd = (row32 % 2 == 1) & inner_lane(lane32, 0)
            dense[pl.ds(32 * s, 32), :] = jnp.where(odd, lane_roll(block, 16), block)
            surf[s, pl.ds(8, 2), :] = block[0:2]
            surf[s, pl.ds(10, 2), :] = block[30:32]
        ghost[pl.ds(0, 128), :] = jnp.dot(
            dense[...], choose, precision=HIGHEST, preferred_element_type=F32
        )
        for s in range(SLOTS):
            block = ghost[pl.ds(32 * s, 32), :]
            block = jnp.where(lane32 // 32 == row32 % 4, block, 0.0)
            block = block + pltpu.roll(block, 31, 0)
            block = block + pltpu.roll(block, 30, 0)
            dense[pl.ds(32 * s, 32), :] = block
            surf[s, pl.ds(0, 8), :] = dense[pl.ds(32 * s, 8, stride=4), :]

        def stage(q, carry):
            slot = slot_of[q]
            flag = jnp.full((8, 128), flag_of[q].astype(F32), F32)
            s_out[q, pl.ds(0, 8), :] = jnp.where(lane8 == 31, flag, surf[slot, pl.ds(0, 8), :])
            s_out[q, pl.ds(8, 4), :] = surf[slot, pl.ds(8, 4), :]
            return carry

        lax.fori_loop(0, members, stage, 0)
        s_in[me] = s_out[me]

    def send_surfaces():
        def send(i, carry):
            q = lax.rem(me + members - i, members)
            pltpu.make_async_remote_copy(
                src_ref=s_out.at[q],
                dst_ref=s_in.at[me],
                send_sem=s_sem.at[0],
                recv_sem=s_sem.at[1],
                device_id=peer(q),
                device_id_type=MESH,
            ).start()
            return carry

        lax.fori_loop(1, members, send, 0)

    def recv_surfaces():
        wait_all(s_in, s_sem.at[1])
        before = jnp.zeros((8, 128), F32)
        tops = [jnp.zeros((8, 128), F32)] * SLOTS
        ends = [jnp.zeros((4, 128), F32)] * SLOTS
        for r in range(members):
            top = s_in[r, pl.ds(0, 8), :]
            end = s_in[r, pl.ds(8, 4), :]
            flag = jnp.sum(jnp.where(lane8 == 31, top, 0.0), axis=1, keepdims=True)
            flag = jnp.broadcast_to(flag, (8, 128))
            mark = jnp.where(flag > 0.5, before, -1.0)
            code[r] = mark
            before = before + flag
            for j in range(SLOTS):
                tops[j] = jnp.where(mark == j, top, tops[j])
                ends[j] = jnp.where(mark[0:4] == j, end, ends[j])
        count[...] = before
        for j in range(SLOTS):
            for i in range(4):
                dense[pl.ds(4 * i + j, 8, stride=16), :] = jnp.where(
                    lane8 // 32 == i, tops[j], 0.0
                )
        i = lax.broadcasted_iota(jnp.int32, (128, 128), 0)
        o = lax.broadcasted_iota(jnp.int32, (128, 128), 1)
        place = (surface_lane(i) == o).astype(F32)
        value = jnp.dot(dense[...], place, precision=HIGHEST, preferred_element_type=F32)
        odd = ((i // 4) % 2 == 1) & inner_lane(o, 112)
        dense[...] = jnp.where(odd, lane_roll(value, 112), value)
        for j in range(SLOTS):
            for y3 in range(2):
                dense[pl.ds(y3 * 4 + j, 1), :] = ends[j][y3 : y3 + 1]
                dense[pl.ds(120 + y3 * 4 + j, 1), :] = ends[j][2 + y3 : 3 + y3]
        spread()

    def wait_all(buffer, sem):
        part = buffer.at[pl.ds(0, members - 1)]
        pltpu.make_async_copy(part, part, sem).wait()

    def recv_parents(c):
        wait_all(d_in.at[c], d_recv.at[c])

        def pick(r8, acc):
            acc = list(acc)
            for r in range(GATHERED):
                r = r8 * GATHERED + r
                mark = code[r]
                for i in range(4):
                    data = d_in[c, r, pl.ds(8 * i, 8), :]
                    for j in range(SLOTS):
                        acc[j * 4 + i] = jnp.where(mark == j, data, acc[j * 4 + i])
            return tuple(acc)

        blank = jnp.zeros((8, 128), F32)
        acc = lax.fori_loop(0, members // GATHERED, pick, (blank,) * 16)
        for j in range(SLOTS):
            for i in range(4):
                dense[pl.ds(32 * i + j, 8, stride=4), :] = acc[j * 4 + i]
        spread()

    def spread():
        for y2 in range(2):
            a = jnp.dot(
                dense[...], expand[:, pl.ds(256 * y2, 128)], precision=HIGHEST,
                preferred_element_type=F32,
            )
            b = jnp.dot(
                dense[...], expand[:, pl.ds(256 * y2 + 128, 128)], precision=HIGHEST,
                preferred_element_type=F32,
            )
            for x in range(16):
                ax, bx = a[8 * x : 8 * x + 8], b[8 * x : 8 * x + 8]
                ghost[pl.ds(x * 32 + y2 * 8, 8), :] = jnp.where(low4, ax, pltpu.roll(bx, 4, 0))
                ghost[pl.ds(x * 32 + 16 + y2 * 8, 8), :] = jnp.where(low4, pltpu.roll(ax, 4, 0), bx)

    fine_y = (row32 // 4) * 4 + lane32 // 32
    fine_z = lane32 % 32
    sides = (
        (fine_y == 0).astype(F32)
        + (fine_y == 31).astype(F32)
        + (fine_z == 0).astype(F32)
        + (fine_z == 31).astype(F32)
    )

    def use_parents(c):
        for X in range(32):
            g = ghost[pl.ds(X // 2 * 32, 32), :]
            times = sides + 1.0 if X in (0, 31) else sides
            fsource[pl.ds(X * 32, 32), :] = fsource[pl.ds(X * 32, 32), :] + times * g

        @pl.when(c > 0)
        def _():
            for X in range(32):
                at = lax.rem(c, 2)
                fine[at, pl.ds(X * 32, 32), :] = (
                    fine[at, pl.ds(X * 32, 32), :] + ghost[pl.ds(X // 2 * 32, 32), :]
                )

    not_first = fine_z > 0
    not_last = fine_z < 31
    first_group = lane32 < 32
    last_group = lane32 >= 96

    def beside(at, X):
        u = fine[at, pl.ds(X * 32, 32), :]
        after = jnp.where(row32 < 28, pltpu.roll(u, 28, 0), 0.0)
        prior = jnp.where(row32 >= 4, pltpu.roll(u, 4, 0), 0.0)
        total = lane_roll(jnp.where(first_group, after, u), -32)
        total = total + lane_roll(jnp.where(last_group, prior, u), 32)
        total = total + lane_roll(jnp.where(not_first, u, 0.0), -1)
        total = total + lane_roll(jnp.where(not_last, u, 0.0), 1)
        if X > 0:
            total = total + fine[at, pl.ds(X * 32 - 32, 32), :]
        if X < 31:
            total = total + fine[at, pl.ds(X * 32 + 32, 32), :]
        return u, total

    def fine_sweeps(c):
        def sweep(s, carry):
            at = lax.rem(c + s, 2)
            for X in range(32):
                u, total = beside(at, X)
                rows = pl.ds(X * 32, 32)
                fine[1 - at, rows, :] = (1.0 - OMEGA) * u + fweight[rows, :] * (fsource[rows, :] + total)
            return carry

        lax.fori_loop(0, FSWEEPS, sweep, 0)

        at = lax.rem(c + FSWEEPS, 2)
        squares = jnp.zeros((8, 128), F32)
        for x in range(16):
            both = None
            for X in (2 * x, 2 * x + 1):
                u, total = beside(at, X)
                rows = pl.ds(X * 32, 32)
                rem = fsource[rows, :] - fdiag[rows, :] * u + total
                sq = rem * rem
                squares = squares + ((sq[0:8] + sq[8:16]) + (sq[16:24] + sq[24:32]))
                both = rem if both is None else both + rem
            for y2 in range(2):
                lo = both[8 * y2 : 8 * y2 + 8]
                hi = both[16 + 8 * y2 : 24 + 8 * y2]
                wide[pl.ds(8 * x, 8), pl.ds(256 * y2, 128)] = jnp.where(low4, lo, pltpu.roll(hi, 4, 0))
                wide[pl.ds(8 * x, 8), pl.ds(256 * y2 + 128, 128)] = jnp.where(
                    low4, pltpu.roll(lo, 4, 0), hi
                )
        live = (sub8 % 4).astype(F32) < count[...]
        fsum[c] = jnp.where(live, squares, 0.0)
        dense[...] = jnp.dot(
            wide[...], gather[...], precision=HIGHEST, preferred_element_type=F32
        )
        for j in range(SLOTS):
            for i in range(4):
                rblocks[j, pl.ds(8 * i, 8), :] = dense[pl.ds(32 * i + j, 8, stride=4), :]

    def send_restricted(c):
        def block_for(r, i):
            mark = code[r]
            value = rblocks[0, pl.ds(8 * i, 8), :]
            for j in range(1, SLOTS):
                value = jnp.where(mark == j, rblocks[j, pl.ds(8 * i, 8), :], value)
            return value

        for i in range(4):
            r_in[c, me, pl.ds(8 * i, 8), :] = block_for(me, i)

        def send(i, carry):
            q = lax.rem(me + members - i, members)
            for part in range(4):
                r_out[c, q, pl.ds(8 * part, 8), :] = block_for(q, part)
            pltpu.make_async_remote_copy(
                src_ref=r_out.at[c, q],
                dst_ref=r_in.at[c, me],
                send_sem=r_send.at[c],
                recv_sem=r_recv.at[c],
                device_id=peer(q),
                device_id_type=MESH,
            ).start()
            return carry

        lax.fori_loop(1, members, send, 0)

    def recv_restricted(c):
        wait_all(r_in.at[c], r_recv.at[c])
        for s in range(SLOTS):
            block = r_in[c, jnp.clip(owners[s], 0, members - 1)]
            for k in range(8):
                value = jnp.where(lane32 // 16 == k, block, 0.0)
                for p, part in enumerate(in_parts(value)):
                    halves[s % 2, pl.ds(k * 32, 32), pl.ds(128 * p, 128)] = part
            placed[s] = jnp.dot(halves[s % 2], lane_out[s], preferred_element_type=F32)
        for by in range(2):
            for k in range(8):
                value = zeros
                for s in range(SLOTS):
                    here = lives[s] & (spots[s] >> 3 == by)
                    value = value + jnp.where(here, placed[s, pl.ds(32 * k, 32), :], 0.0)
                mixed[pl.ds(k * PITCH + by * 32, 32), :] = value
        for x in range(16):
            for t in range(4):
                rows = pl.ds(x * 32 + 8 * t, 8)
                comp[rows, :] = (
                    source[rows, :]
                    + mixed[pl.ds(t // 2 * 32 + x * 2 + t % 2, 8, stride=PITCH), :]
                )

    edge_lane = (lane8 == 0) | (lane8 == 127)

    def coarse_inner(k):
        for x in range(16):
            p = pot[k, pl.ds(x * 32, 32), :]
            total = jnp.where(row32 < 31, pltpu.roll(p, 31, 0), 0.0)
            total = total + jnp.where(row32 > 0, pltpu.roll(p, 1, 0), 0.0)
            total = total + jnp.where(lane32 < 127, lane_roll(p, -1), 0.0)
            total = total + jnp.where(lane32 > 0, lane_roll(p, 1), 0.0)
            if x > 0:
                total = total + pot[k, pl.ds(x * 32 - 32, 32), :]
            if x < 15:
                total = total + pot[k, pl.ds(x * 32 + 32, 32), :]
            beside_sum[pl.ds(x * 32, 32), :] = total

    def coarse_sweep(c, k, last):
        halo(k, range(6), "recv")
        beyond = jnp.where(
            lane8 % 2 == 0,
            jnp.where(gz > 0, lane_roll(zlo[k], 1), 0.0),
            jnp.where(gz < n_z - 1, lane_roll(zhi[k], -1), 0.0),
        )
        acc = jnp.zeros((8, 128), F32)
        squares = jnp.zeros((8, 128), F32)
        for x in [0, 15] + list(range(1, 15)):
            rows = pl.ds(x * 32, 32)
            p = pot[k, rows, :]
            total = comp[rows, :] + beside_sum[rows, :]
            if x == 0:
                total = total + jnp.where(gx > 0, xlo[k], 0.0)
            if x == 15:
                total = total + jnp.where(gx < n_x - 1, xhi[k], 0.0)
            above = jnp.where(gy < n_y - 1, yhi[k, pl.ds(x, 1), :], 0.0)
            below = jnp.where(gy > 0, ylo[k, pl.ds(x, 1), :], 0.0)
            parts = []
            for t in range(4):
                edge = lane_roll(beyond, -2 * (x * 4 + t))
                part = total[8 * t : 8 * t + 8] + jnp.where(edge_lane, edge, 0.0)
                if t == 0:
                    part = part + jnp.where(sub8 == 0, jnp.broadcast_to(below, (8, 128)), 0.0)
                if t == 3:
                    part = part + jnp.where(sub8 == 7, jnp.broadcast_to(above, (8, 128)), 0.0)
                parts.append(part)
            total = jnp.concatenate(parts, axis=0)
            if last:
                res = total - diag[rows, :] * p
                sq = res * res
                squares = squares + ((sq[0:8] + sq[8:16]) + (sq[16:24] + sq[24:32]))
                new = p + weight[rows, :] * res
            else:
                new = (1.0 - OMEGA) * p + weight[rows, :] * total
            pot[k + 1, rows, :] = new
            acc = faces_of(x, new, k + 1, acc)
            if x == 15:
                halo(k + 1, (0, 1), "start")
        zface[k + 1] = acc
        halo(k + 1, (2, 3, 4, 5), "start")
        if last:
            csum[c] = squares

    loads[0].wait()
    acc = jnp.zeros((8, 128), F32)
    for x in range(16):
        acc = faces_of(x, pot[0, pl.ds(x * 32, 32), :], 0, acc)
    zface[0] = acc
    stage_surfaces()
    pl.semaphore_wait(barrier, members + 1)
    send_surfaces()
    halo(0, range(6), "start")

    rounds = []
    while 2 ** len(rounds) * 2 <= n_x // 2:
        rounds.append(2 ** len(rounds))

    def chain_step(at):
        if 0 < at <= len(rounds):
            pl.semaphore_wait(chain.at[at - 1], 2)
        if at < len(rounds):
            for way in (1, -1):
                pl.semaphore_signal(
                    chain.at[at],
                    inc=1,
                    device_id={"gx": ring(way * rounds[at])},
                    device_id_type=MESH,
                )

    chain_step(0)

    def prepare():
        i = lax.broadcasted_iota(jnp.int32, (128, 512), 0)
        n = lax.broadcasted_iota(jnp.int32, (128, 512), 1)
        lane = n % 128
        expand[...] = (i == (n // 128) * 32 + (lane // 64) * 16 + (lane % 32) // 2).astype(F32)
        n = lax.broadcasted_iota(jnp.int32, (512, 128), 0)
        o = lax.broadcasted_iota(jnp.int32, (512, 128), 1)
        lane = n % 128
        gather[...] = jnp.where(
            o == (n // 128) * 32 + (lane // 64) * 16 + (lane % 32) // 2, 0.125, 0.0
        )
        loads[2].wait()
        for x in range(16):
            rows = pl.ds(x * 32, 32)
            d = 6.0 + diag[rows, :]
            diag[rows, :] = d
            weight[rows, :] = OMEGA / d
        loads[4].wait()
        for X in range(32):
            rows = pl.ds(X * 32, 32)
            d = 6.0 + fdiag[rows, :]
            fdiag[rows, :] = d
            fweight[rows, :] = OMEGA / d
        for at in (1, 3, 5):
            loads[at].wait()

    norm_row = lax.broadcasted_iota(jnp.int32, (1, 128), 1)

    def norm_copy(src, dst, sem, device):
        return pltpu.make_async_remote_copy(
            src_ref=src,
            dst_ref=dst,
            send_sem=n_sem.at[sem],
            recv_sem=n_sem.at[sem + 1],
            device_id=device,
            device_id_type=MESH,
        )

    def send_norms():
        parts = [jnp.sum(csum[k] + fsum[k]) for k in range(CYCLES)]
        row = jnp.where(norm_row < 64, parts[0], parts[1])
        n_send[0] = row
        nx_in[gx] = row

        for i in sorted(range(1, n_x), key=lambda d: -min(d, n_x - d)):
            norm_copy(n_send.at[0], nx_in.at[gx], 0, {"gx": lax.rem(gx + i, n_x)}).start()

    def turn_norms():
        part = nx_in.at[pl.ds(0, n_x - 1)]
        pltpu.make_async_copy(part, part, n_sem.at[1]).wait()
        row = nx_in[0]
        for r in range(1, n_x):
            row = row + nx_in[r]
        n_send[1] = row
        np_in[me] = row

        def send(i, carry):
            norm_copy(n_send.at[1], np_in.at[me], 2, peer(lax.rem(me + i, members))).start()
            return carry

        lax.fori_loop(1, members, send, 0)

    def end_norms():
        wait_all(np_in, n_sem.at[3])
        row = np_in[0]
        for r in range(1, members):
            row = row + np_in[r]
        row = jnp.sqrt(row / cells)
        for k in range(CYCLES):
            norm_out[k] = row[0, 64 * k]

    def cycle(c, carry):
        use_parents(c)
        for k in range(CYCLES):

            @pl.when(c == k)
            def _(k=k):
                chain_step(2 * k + 1)

        fine_sweeps(c)
        send_restricted(c)
        for k in range(CYCLES):

            @pl.when(c == k)
            def _(k=k):
                chain_step(2 * k + 2)

        recv_restricted(c)

        def sweep(s, carry):
            coarse_sweep(c, c * CSWEEPS + s, False)
            coarse_inner(c * CSWEEPS + s + 1)
            return carry

        lax.fori_loop(0, CSWEEPS - 1, sweep, 0)
        coarse_sweep(c, c * CSWEEPS + CSWEEPS - 1, True)

        @pl.when(c == CYCLES - 1)
        def _():
            send_norms()

        send_parents(c)
        coarse_inner(c * CSWEEPS + CSWEEPS)
        recv_parents(c)
        return carry

    prepare()
    coarse_inner(0)
    recv_surfaces()
    lax.fori_loop(0, CYCLES, cycle, 0)

    pot_out[...] = pot[SWEEPS]
    live = ((row32 % 4).astype(F32) < jnp.concatenate([count[...]] * 4, axis=0)).astype(F32)
    end = CYCLES % 2
    for X in range(32):
        rows = pl.ds(X * 32, 32)
        fine_out[rows, :] = (fine[end, rows, :] + ghost[pl.ds(X // 2 * 32, 32), :]) * live
    turn_norms()

    wait_all(s_out, s_sem.at[0])
    for c in range(CYCLES):
        wait_all(d_out.at[c], d_send.at[c])
        wait_all(r_out.at[c], r_send.at[c])
    halo(SWEEPS, range(6), "recv")

    def left(k, carry):
        halo(k, range(6), "send")
        return carry

    lax.fori_loop(0, SWEEPS + 1, left, 0)
    part = nx_in.at[pl.ds(0, n_x - 1)]
    pltpu.make_async_copy(part, part, n_sem.at[0]).wait()
    end_norms()
    wait_all(np_in, n_sem.at[2])


def local(
    coarse_source,
    coarse_shift,
    coarse_start,
    fine_source,
    fine_shift,
    fine_start,
    box_corner,
    box_owner,
):
    n_x, n_y, n_z = (lax.axis_size(a) for a in ("gx", "gy", "gz"))
    members = n_y * n_z
    cells = float(n_x * n_y * n_z * coarse_source.size)

    def fine_rows(array):
        return array.reshape(SLOTS, 256, 128).transpose(1, 0, 2).reshape(FROWS, 128)

    hbm = pl.BlockSpec(memory_space=pltpu.HBM)
    smem = pl.BlockSpec(memory_space=pltpu.SMEM)
    vmem = pl.BlockSpec(memory_space=pltpu.VMEM)

    def buf(*shape):
        return pltpu.VMEM(shape, F32)

    sems = pltpu.SemaphoreType.DMA
    pot, fine, norms = pl.pallas_call(
        functools.partial(kernel, (n_x, n_y, n_z, cells)),
        out_shape=(
            jax.ShapeDtypeStruct((ROWS, 128), F32),
            jax.ShapeDtypeStruct((FROWS, 128), F32),
            jax.ShapeDtypeStruct((CYCLES,), F32),
        ),
        in_specs=[hbm] * 8,
        out_specs=(vmem, vmem, smem),
        scratch_shapes=[
            buf(SWEEPS + 1, ROWS, 128),
            buf(ROWS, 128),
            buf(ROWS, 128),
            buf(ROWS, 128),
            buf(ROWS, 128),
            buf(ROWS, 128),
            buf(SWEEPS + 1, 32, 128),
            buf(SWEEPS + 1, 32, 128),
            buf(SWEEPS + 1, 16, 128),
            buf(SWEEPS + 1, 16, 128),
            buf(SWEEPS + 1, 8, 128),
            buf(SWEEPS + 1, 8, 128),
            buf(SWEEPS + 1, 2, 16, 128),
            buf(SWEEPS + 1, 8, 128),
            buf(2, FROWS, 128),
            buf(FROWS, 128),
            buf(FROWS, 128),
            buf(FROWS, 128),
            buf(128, 512),
            buf(512, 128),
            buf(128, 128),
            buf(ROWS, 128),
            buf(128, 512),
            buf(SLOTS, 32, 128),
            pltpu.VMEM((2, 256, 384), jnp.bfloat16),
            buf(SLOTS, 256, 128),
            pltpu.VMEM((SLOTS, 384, 128), jnp.bfloat16),
            pltpu.VMEM((SLOTS, 384, 128), jnp.bfloat16),
            buf(8 * PITCH, 128),
            buf(SLOTS, 32, 128),
            buf(members, 8, 128),
            buf(8, 128),
            pltpu.SMEM((3, 1, SLOTS), jnp.int32),
            pltpu.SMEM((1, SLOTS), jnp.int32),
            pltpu.SMEM((members,), jnp.int32),
            pltpu.SMEM((members,), jnp.int32),
            buf(SLOTS, 12, 128),
            buf(members, 12, 128),
            buf(members, 12, 128),
            buf(CYCLES, members, 32, 128),
            buf(CYCLES, members, 32, 128),
            buf(CYCLES, members, 32, 128),
            buf(CYCLES, members, 32, 128),
            buf(CYCLES, 8, 128),
            buf(CYCLES, 8, 128),
            buf(n_x, 1, 128),
            buf(members, 1, 128),
            buf(2, 1, 128),
            sems((8,)),
            sems((2,)),
            sems((CYCLES,)),
            sems((CYCLES,)),
            sems((CYCLES,)),
            sems((CYCLES,)),
            sems((SWEEPS + 1, 6)),
            sems((SWEEPS + 1, 6)),
            sems((4,)),
            pltpu.SemaphoreType.REGULAR((4,)),
        ],
        compiler_params=pltpu.CompilerParams(
            collective_id=0, has_side_effects=True, vmem_limit_bytes=30 * 1000 * 1000
        ),
        name="cycles",
    )(
        *(
            pltpu.with_memory_space_constraint(array, pltpu.HBM)
            for array in (
                box_corner.transpose(2, 0, 1),
                box_owner,
                coarse_source.reshape(ROWS, 128),
                coarse_shift.reshape(ROWS, 128),
                coarse_start.reshape(ROWS, 128),
                fine_rows(fine_source),
                fine_rows(fine_shift),
                fine_rows(fine_start),
            )
        ),
    )
    fine = fine.reshape(256, SLOTS, 128).transpose(1, 0, 2).reshape(SLOTS, 256 * 128)
    return pot.reshape(coarse_source.shape), fine, norms


def solution(mesh):
    every = ("gx", "gy", "gz")
    return jax.shard_map(
        local,
        mesh=mesh,
        in_specs=(
            P("gx", "gy", "gz"),
            P("gx", "gy", "gz"),
            P("gx", "gy", "gz"),
            P(every, None),
            P(every, None),
            P(every, None),
            P(every, None, None),
            P(every, None),
        ),
        out_specs=(P("gx", "gy", "gz"), P(every, None), P()),
        check_vma=False,
    )
```

```python
import functools

import jax
import jax.numpy as jnp
from jax import lax
from jax.experimental import pallas as pl
from jax.experimental.pallas import tpu as pltpu
from jax.sharding import PartitionSpec as P

FOOT = 16
CYCLES = 2
CSWEEPS = 4
FSWEEPS = 3
SLOTS = 4
OMEGA = 0.8
HIGHEST = lax.Precision.HIGHEST
F32 = jnp.float32
MESH = pl.DeviceIdType.MESH

ROWS = 512
FROWS = 1024
SWEEPS = CYCLES * CSWEEPS
GATHERED = 4
PITCH = 72


def lane_roll(array, shift):
    return pltpu.roll(array, shift % 128, 1)


def far_first(n_y, n_z):
    def hops(offset):
        return min(offset[0], n_y // 2 - offset[0]) + min(offset[2], n_z - offset[2])

    def link(offset):
        dy, _, dz = offset
        return (0, dz <= n_z // 2) if dz else (1, dy <= n_y // 4) if dy else (2, True)

    queues = {}
    every = [(y, c, z) for y in range(n_y // 2) for c in range(2) for z in range(n_z)][1:]
    for offset in sorted(every, key=lambda o: -hops(o)):
        queues.setdefault(link(offset), []).append(offset)
    order = []
    while any(queues.values()):
        order += [queue.pop(0) for queue in queues.values() if queue]
    return order


def in_parts(value):
    parts = []
    for _ in range(3):
        cut = value.astype(jnp.bfloat16)
        parts.append(cut)
        value = value - cut.astype(F32)
    return parts


def kernel(
    sizes,
    corner_hbm,
    owner_hbm,
    source_hbm,
    shift_hbm,
    start_hbm,
    fsource_hbm,
    fshift_hbm,
    fstart_hbm,
    pot_out,
    fine_out,
    norm_out,
    pot,
    source,
    diag,
    weight,
    comp,
    beside_sum,
    xlo,
    xhi,
    ylo,
    yhi,
    zlo,
    zhi,
    yface,
    zface,
    fine,
    fsource,
    fdiag,
    fweight,
    expand,
    gather,
    dense,
    ghost,
    wide,
    packed,
    halves,
    placed,
    lane_in,
    lane_out,
    mixed,
    rblocks,
    code,
    count,
    corner,
    owner,
    slot_of,
    flag_of,
    surf,
    s_out,
    s_in,
    d_out,
    d_in,
    r_out,
    r_in,
    csum,
    fsum,
    nx_in,
    np_in,
    n_send,
    local_sem,
    s_sem,
    d_send,
    d_recv,
    r_send,
    r_recv,
    h_send,
    h_recv,
    n_sem,
    chain,
):
    n_x, n_y, n_z, cells = sizes
    members = n_y * n_z
    gx, gy, gz = lax.axis_index("gx"), lax.axis_index("gy"), lax.axis_index("gz")
    me = gy * n_z + gz

    def others():
        for dy, dc, dz in far_first(n_y, n_z):
            y = lax.rem(gy // 2 + dy, n_y // 2) * 2 + lax.rem(gy + dc, 2)
            yield y * n_z + lax.rem(gz + dz, n_z)

    def peer(q):
        return {"gy": q // n_z, "gz": lax.rem(q, n_z)}

    barrier = pltpu.get_barrier_semaphore()

    def greet(i, carry):
        q = lax.rem(me + i, members)
        pl.semaphore_signal(barrier, inc=1, device_id=peer(q), device_id_type=MESH)
        return carry

    lax.fori_loop(1, members, greet, 0)

    def ring(distance):
        return lax.rem(gx + distance + n_x, n_x)

    for way in (1, -1):
        pl.semaphore_signal(barrier, inc=1, device_id={"gx": ring(way)}, device_id_type=MESH)

    tables = [
        pltpu.make_async_copy(corner_hbm, corner, local_sem.at[6]),
        pltpu.make_async_copy(owner_hbm, owner, local_sem.at[7]),
    ]
    loads = [
        pltpu.make_async_copy(start_hbm, pot.at[0], local_sem.at[0]),
        pltpu.make_async_copy(source_hbm, source, local_sem.at[1]),
        pltpu.make_async_copy(shift_hbm, diag, local_sem.at[2]),
        pltpu.make_async_copy(fsource_hbm, fsource, local_sem.at[3]),
        pltpu.make_async_copy(fshift_hbm, fdiag, local_sem.at[4]),
        pltpu.make_async_copy(fstart_hbm, fine.at[0], local_sem.at[5]),
    ]
    for load in tables + loads:
        load.start()

    for table in tables:
        table.wait()
    owners = [owner[0, s] for s in range(SLOTS)]
    lives = [(o >= 0) & (o < members) for o in owners]
    places = [
        jnp.where(
            lives[s],
            ((corner[1, 0, s] >> 5) & 1) * 8 + ((corner[2, 0, s] >> 5) & 7),
            -1,
        )
        for s in range(SLOTS)
    ]
    spots = [jnp.maximum(place, 0) for place in places]
    for q in range(members):
        slot = jnp.int32(0)
        flag = jnp.int32(0)
        for s in range(SLOTS):
            mine = owners[s] == q
            slot = jnp.where(mine, s, slot)
            flag = jnp.where(mine, 1, flag)
        slot_of[q] = slot
        flag_of[q] = flag
    i = lax.broadcasted_iota(jnp.int32, (384, 128), 0) % 128
    o = lax.broadcasted_iota(jnp.int32, (384, 128), 1)
    for s in range(SLOTS):
        group = spots[s] & 7
        lane_in[s] = ((i % 16 == o % 16) & (i // 16 == group)).astype(F32).astype(jnp.bfloat16)
        lane_out[s] = ((i % 16 == o % 16) & (o // 16 == group)).astype(F32).astype(jnp.bfloat16)

    lane8 = lax.broadcasted_iota(jnp.int32, (8, 128), 1)
    sub8 = lax.broadcasted_iota(jnp.int32, (8, 128), 0)
    lane32 = lax.broadcasted_iota(jnp.int32, (32, 128), 1)
    row32 = lax.broadcasted_iota(jnp.int32, (32, 128), 0)
    low4 = sub8 < 4

    zeros = jnp.zeros((32, 128), F32)

    def halo(k, sides, act):
        routes = (
            (pot.at[k, pl.ds(0, 32)], xhi.at[k], {"gx": ring(-1)}),
            (pot.at[k, pl.ds(ROWS - 32, 32)], xlo.at[k], {"gx": ring(1)}),
            (yface.at[k, 0], yhi.at[k], {"gy": lax.rem(gy + n_y - 1, n_y)}),
            (yface.at[k, 1], ylo.at[k], {"gy": lax.rem(gy + 1, n_y)}),
            (zface.at[k], zhi.at[k], {"gz": lax.rem(gz + n_z - 1, n_z)}),
            (zface.at[k], zlo.at[k], {"gz": lax.rem(gz + 1, n_z)}),
        )
        for i in sides:
            src, dst, device = routes[i]
            copy = pltpu.make_async_remote_copy(
                src_ref=src,
                dst_ref=dst,
                send_sem=h_send.at[k, i],
                recv_sem=h_recv.at[k, i],
                device_id=device,
                device_id_type=MESH,
            )
            if act == "start":
                copy.start()
            elif act == "recv":
                copy.wait_recv()
            else:
                copy.wait_send()

    def faces_of(x, slab, k, acc):
        yface[k, 0, pl.ds(x, 1), :] = slab[0:1]
        yface[k, 1, pl.ds(x, 1), :] = slab[31:32]
        for t in range(4):
            v = x * 4 + t
            keep = (lane8 == 2 * v) | (lane8 == (2 * v - 1) % 128)
            acc = jnp.where(keep, lane_roll(slab[8 * t : 8 * t + 8], 2 * v), acc)
        return acc

    def pack_parents(slab_of):
        for x in range(16):
            slab = slab_of(x)
            for by in range(2):
                for y3 in range(2):
                    t = by * 2 + y3
                    mixed[pl.ds(by * 32 + x * 2 + y3, 8, stride=PITCH), :] = slab[8 * t : 8 * t + 8]
        for by in range(2):
            for k in range(8):
                value = mixed[pl.ds(k * PITCH + by * 32, 32), :]
                for p, part in enumerate(in_parts(value)):
                    halves[by, pl.ds(k * 32, 32), pl.ds(128 * p, 128)] = part
        for s in range(SLOTS):
            rows = jnp.dot(
                halves[spots[s] >> 3], lane_in[s], preferred_element_type=F32
            )
            value = rows[0:32]
            for k in range(1, 8):
                value = jnp.where(lane32 // 16 == k, rows[32 * k : 32 * k + 32], value)
            packed[s] = value

    def send_parents(c):
        rows_of = lambda at, x: pot[at, pl.ds(x * 32, 32), :]
        pack_parents(lambda x: rows_of(c * CSWEEPS + CSWEEPS, x) - rows_of(c * CSWEEPS, x))
        d_in[c, me] = packed[slot_of[me]]

        def send(q):
            d_out[c, q] = packed[slot_of[q]]
            pltpu.make_async_remote_copy(
                src_ref=d_out.at[c, q],
                dst_ref=d_in.at[c, me],
                send_sem=d_send.at[c],
                recv_sem=d_recv.at[c],
                device_id=peer(q),
                device_id_type=MESH,
            ).start()

        for q in others():
            send(q)

    inner_lane = lambda lane, first: (lane > first) & (lane < first + 15)

    def surface_lane(o):
        m = o % 32
        at = jnp.where(m < 16, m, ((m - 16) // 2 + 1) * 16 + (m % 2) * 15)
        return jnp.where(m < 30, at, -1)

    def stage_surfaces():
        pack_parents(lambda x: pot[0, pl.ds(x * 32, 32), :])
        i = lax.broadcasted_iota(jnp.int32, (128, 128), 0)
        o = lax.broadcasted_iota(jnp.int32, (128, 128), 1)
        choose = (i == surface_lane(o)).astype(F32)
        for s in range(SLOTS):
            block = packed[s]
            odd = (row32 % 2 == 1) & inner_lane(lane32, 0)
            dense[pl.ds(32 * s, 32), :] = jnp.where(odd, lane_roll(block, 16), block)
            surf[s, pl.ds(8, 2), :] = block[0:2]
            surf[s, pl.ds(10, 2), :] = block[30:32]
        ghost[pl.ds(0, 128), :] = jnp.dot(
            dense[...], choose, precision=HIGHEST, preferred_element_type=F32
        )
        for s in range(SLOTS):
            block = ghost[pl.ds(32 * s, 32), :]
            block = jnp.where(lane32 // 32 == row32 % 4, block, 0.0)
            block = block + pltpu.roll(block, 31, 0)
            block = block + pltpu.roll(block, 30, 0)
            dense[pl.ds(32 * s, 32), :] = block
            surf[s, pl.ds(0, 8), :] = dense[pl.ds(32 * s, 8, stride=4), :]

        def stage(q, carry):
            slot = slot_of[q]
            flag = jnp.full((8, 128), flag_of[q].astype(F32), F32)
            s_out[q, pl.ds(0, 8), :] = jnp.where(lane8 == 31, flag, surf[slot, pl.ds(0, 8), :])
            s_out[q, pl.ds(8, 4), :] = surf[slot, pl.ds(8, 4), :]
            return carry

        lax.fori_loop(0, members, stage, 0)
        s_in[me] = s_out[me]

    def send_surfaces():
        def send(q):
            pltpu.make_async_remote_copy(
                src_ref=s_out.at[q],
                dst_ref=s_in.at[me],
                send_sem=s_sem.at[0],
                recv_sem=s_sem.at[1],
                device_id=peer(q),
                device_id_type=MESH,
            ).start()

        for q in others():
            send(q)

    def recv_surfaces():
        wait_all(s_in, s_sem.at[1])
        before = jnp.zeros((8, 128), F32)
        tops = [jnp.zeros((8, 128), F32)] * SLOTS
        ends = [jnp.zeros((4, 128), F32)] * SLOTS
        for r in range(members):
            top = s_in[r, pl.ds(0, 8), :]
            end = s_in[r, pl.ds(8, 4), :]
            flag = jnp.sum(jnp.where(lane8 == 31, top, 0.0), axis=1, keepdims=True)
            flag = jnp.broadcast_to(flag, (8, 128))
            mark = jnp.where(flag > 0.5, before, -1.0)
            code[r] = mark
            before = before + flag
            for j in range(SLOTS):
                tops[j] = jnp.where(mark == j, top, tops[j])
                ends[j] = jnp.where(mark[0:4] == j, end, ends[j])
        count[...] = before
        for j in range(SLOTS):
            for i in range(4):
                dense[pl.ds(4 * i + j, 8, stride=16), :] = jnp.where(
                    lane8 // 32 == i, tops[j], 0.0
                )
        i = lax.broadcasted_iota(jnp.int32, (128, 128), 0)
        o = lax.broadcasted_iota(jnp.int32, (128, 128), 1)
        place = (surface_lane(i) == o).astype(F32)
        value = jnp.dot(dense[...], place, precision=HIGHEST, preferred_element_type=F32)
        odd = ((i // 4) % 2 == 1) & inner_lane(o, 112)
        dense[...] = jnp.where(odd, lane_roll(value, 112), value)
        for j in range(SLOTS):
            for y3 in range(2):
                dense[pl.ds(y3 * 4 + j, 1), :] = ends[j][y3 : y3 + 1]
                dense[pl.ds(120 + y3 * 4 + j, 1), :] = ends[j][2 + y3 : 3 + y3]
        spread()

    def wait_all(buffer, sem):
        part = buffer.at[pl.ds(0, members - 1)]
        pltpu.make_async_copy(part, part, sem).wait()

    def recv_parents(c):
        wait_all(d_in.at[c], d_recv.at[c])

        def pick(r8, acc):
            acc = list(acc)
            for r in range(GATHERED):
                r = r8 * GATHERED + r
                mark = code[r]
                for i in range(4):
                    data = d_in[c, r, pl.ds(8 * i, 8), :]
                    for j in range(SLOTS):
                        acc[j * 4 + i] = jnp.where(mark == j, data, acc[j * 4 + i])
            return tuple(acc)

        blank = jnp.zeros((8, 128), F32)
        acc = lax.fori_loop(0, members // GATHERED, pick, (blank,) * 16)
        for j in range(SLOTS):
            for i in range(4):
                dense[pl.ds(32 * i + j, 8, stride=4), :] = acc[j * 4 + i]
        spread()

    def spread():
        for y2 in range(2):
            a = jnp.dot(
                dense[...], expand[:, pl.ds(256 * y2, 128)], precision=HIGHEST,
                preferred_element_type=F32,
            )
            b = jnp.dot(
                dense[...], expand[:, pl.ds(256 * y2 + 128, 128)], precision=HIGHEST,
                preferred_element_type=F32,
            )
            for x in range(16):
                ax, bx = a[8 * x : 8 * x + 8], b[8 * x : 8 * x + 8]
                ghost[pl.ds(x * 32 + y2 * 8, 8), :] = jnp.where(low4, ax, pltpu.roll(bx, 4, 0))
                ghost[pl.ds(x * 32 + 16 + y2 * 8, 8), :] = jnp.where(low4, pltpu.roll(ax, 4, 0), bx)

    fine_y = (row32 // 4) * 4 + lane32 // 32
    fine_z = lane32 % 32
    sides = (
        (fine_y == 0).astype(F32)
        + (fine_y == 31).astype(F32)
        + (fine_z == 0).astype(F32)
        + (fine_z == 31).astype(F32)
    )

    def use_parents(c):
        for X in range(32):
            g = ghost[pl.ds(X // 2 * 32, 32), :]
            times = sides + 1.0 if X in (0, 31) else sides
            fsource[pl.ds(X * 32, 32), :] = fsource[pl.ds(X * 32, 32), :] + times * g

        @pl.when(c > 0)
        def _():
            for X in range(32):
                at = lax.rem(c, 2)
                fine[at, pl.ds(X * 32, 32), :] = (
                    fine[at, pl.ds(X * 32, 32), :] + ghost[pl.ds(X // 2 * 32, 32), :]
                )

    not_first = fine_z > 0
    not_last = fine_z < 31
    first_group = lane32 < 32
    last_group = lane32 >= 96

    def beside(at, X):
        u = fine[at, pl.ds(X * 32, 32), :]
        after = jnp.where(row32 < 28, pltpu.roll(u, 28, 0), 0.0)
        prior = jnp.where(row32 >= 4, pltpu.roll(u, 4, 0), 0.0)
        total = lane_roll(jnp.where(first_group, after, u), -32)
        total = total + lane_roll(jnp.where(last_group, prior, u), 32)
        total = total + lane_roll(jnp.where(not_first, u, 0.0), -1)
        total = total + lane_roll(jnp.where(not_last, u, 0.0), 1)
        if X > 0:
            total = total + fine[at, pl.ds(X * 32 - 32, 32), :]
        if X < 31:
            total = total + fine[at, pl.ds(X * 32 + 32, 32), :]
        return u, total

    def fine_sweeps(c):
        def sweep(s, carry):
            at = lax.rem(c + s, 2)
            for X in range(32):
                u, total = beside(at, X)
                rows = pl.ds(X * 32, 32)
                fine[1 - at, rows, :] = (1.0 - OMEGA) * u + fweight[rows, :] * (fsource[rows, :] + total)
            return carry

        lax.fori_loop(0, FSWEEPS, sweep, 0)

        at = lax.rem(c + FSWEEPS, 2)
        squares = jnp.zeros((8, 128), F32)
        for x in range(16):
            both = None
            for X in (2 * x, 2 * x + 1):
                u, total = beside(at, X)
                rows = pl.ds(X * 32, 32)
                rem = fsource[rows, :] - fdiag[rows, :] * u + total
                sq = rem * rem
                squares = squares + ((sq[0:8] + sq[8:16]) + (sq[16:24] + sq[24:32]))
                both = rem if both is None else both + rem
            for y2 in range(2):
                lo = both[8 * y2 : 8 * y2 + 8]
                hi = both[16 + 8 * y2 : 24 + 8 * y2]
                wide[pl.ds(8 * x, 8), pl.ds(256 * y2, 128)] = jnp.where(low4, lo, pltpu.roll(hi, 4, 0))
                wide[pl.ds(8 * x, 8), pl.ds(256 * y2 + 128, 128)] = jnp.where(
                    low4, pltpu.roll(lo, 4, 0), hi
                )
        live = (sub8 % 4).astype(F32) < count[...]
        fsum[c] = jnp.where(live, squares, 0.0)
        dense[...] = jnp.dot(
            wide[...], gather[...], precision=HIGHEST, preferred_element_type=F32
        )
        for j in range(SLOTS):
            for i in range(4):
                rblocks[j, pl.ds(8 * i, 8), :] = dense[pl.ds(32 * i + j, 8, stride=4), :]

    def send_restricted(c):
        def block_for(r, i):
            mark = code[r]
            value = rblocks[0, pl.ds(8 * i, 8), :]
            for j in range(1, SLOTS):
                value = jnp.where(mark == j, rblocks[j, pl.ds(8 * i, 8), :], value)
            return value

        for i in range(4):
            r_in[c, me, pl.ds(8 * i, 8), :] = block_for(me, i)

        def send(q):
            for part in range(4):
                r_out[c, q, pl.ds(8 * part, 8), :] = block_for(q, part)
            pltpu.make_async_remote_copy(
                src_ref=r_out.at[c, q],
                dst_ref=r_in.at[c, me],
                send_sem=r_send.at[c],
                recv_sem=r_recv.at[c],
                device_id=peer(q),
                device_id_type=MESH,
            ).start()

        for q in others():
            send(q)

    def recv_restricted(c):
        wait_all(r_in.at[c], r_recv.at[c])
        for s in range(SLOTS):
            block = r_in[c, jnp.clip(owners[s], 0, members - 1)]
            for k in range(8):
                value = jnp.where(lane32 // 16 == k, block, 0.0)
                for p, part in enumerate(in_parts(value)):
                    halves[s % 2, pl.ds(k * 32, 32), pl.ds(128 * p, 128)] = part
            placed[s] = jnp.dot(halves[s % 2], lane_out[s], preferred_element_type=F32)
        for by in range(2):
            for k in range(8):
                value = zeros
                for s in range(SLOTS):
                    here = lives[s] & (spots[s] >> 3 == by)
                    value = value + jnp.where(here, placed[s, pl.ds(32 * k, 32), :], 0.0)
                mixed[pl.ds(k * PITCH + by * 32, 32), :] = value
        for x in range(16):
            for t in range(4):
                rows = pl.ds(x * 32 + 8 * t, 8)
                comp[rows, :] = (
                    source[rows, :]
                    + mixed[pl.ds(t // 2 * 32 + x * 2 + t % 2, 8, stride=PITCH), :]
                )

    edge_lane = (lane8 == 0) | (lane8 == 127)

    def coarse_inner(k):
        for x in range(16):
            p = pot[k, pl.ds(x * 32, 32), :]
            total = jnp.where(row32 < 31, pltpu.roll(p, 31, 0), 0.0)
            total = total + jnp.where(row32 > 0, pltpu.roll(p, 1, 0), 0.0)
            total = total + jnp.where(lane32 < 127, lane_roll(p, -1), 0.0)
            total = total + jnp.where(lane32 > 0, lane_roll(p, 1), 0.0)
            if x > 0:
                total = total + pot[k, pl.ds(x * 32 - 32, 32), :]
            if x < 15:
                total = total + pot[k, pl.ds(x * 32 + 32, 32), :]
            beside_sum[pl.ds(x * 32, 32), :] = total

    def coarse_sweep(c, k, last):
        halo(k, range(6), "recv")
        beyond = jnp.where(
            lane8 % 2 == 0,
            jnp.where(gz > 0, lane_roll(zlo[k], 1), 0.0),
            jnp.where(gz < n_z - 1, lane_roll(zhi[k], -1), 0.0),
        )
        acc = jnp.zeros((8, 128), F32)
        squares = jnp.zeros((8, 128), F32)
        for x in [0, 15] + list(range(1, 15)):
            rows = pl.ds(x * 32, 32)
            p = pot[k, rows, :]
            total = comp[rows, :] + beside_sum[rows, :]
            if x == 0:
                total = total + jnp.where(gx > 0, xlo[k], 0.0)
            if x == 15:
                total = total + jnp.where(gx < n_x - 1, xhi[k], 0.0)
            above = jnp.where(gy < n_y - 1, yhi[k, pl.ds(x, 1), :], 0.0)
            below = jnp.where(gy > 0, ylo[k, pl.ds(x, 1), :], 0.0)
            parts = []
            for t in range(4):
                edge = lane_roll(beyond, -2 * (x * 4 + t))
                part = total[8 * t : 8 * t + 8] + jnp.where(edge_lane, edge, 0.0)
                if t == 0:
                    part = part + jnp.where(sub8 == 0, jnp.broadcast_to(below, (8, 128)), 0.0)
                if t == 3:
                    part = part + jnp.where(sub8 == 7, jnp.broadcast_to(above, (8, 128)), 0.0)
                parts.append(part)
            total = jnp.concatenate(parts, axis=0)
            if last:
                res = total - diag[rows, :] * p
                sq = res * res
                squares = squares + ((sq[0:8] + sq[8:16]) + (sq[16:24] + sq[24:32]))
                new = p + weight[rows, :] * res
            else:
                new = (1.0 - OMEGA) * p + weight[rows, :] * total
            pot[k + 1, rows, :] = new
            acc = faces_of(x, new, k + 1, acc)
            if x == 15:
                halo(k + 1, (0, 1), "start")
        zface[k + 1] = acc
        halo(k + 1, (2, 3, 4, 5), "start")
        if last:
            csum[c] = squares

    loads[0].wait()
    acc = jnp.zeros((8, 128), F32)
    for x in range(16):
        acc = faces_of(x, pot[0, pl.ds(x * 32, 32), :], 0, acc)
    zface[0] = acc
    stage_surfaces()
    pl.semaphore_wait(barrier, members + 1)
    send_surfaces()
    halo(0, range(6), "start")

    rounds = []
    while 2 ** len(rounds) * 2 <= n_x // 2:
        rounds.append(2 ** len(rounds))

    def chain_step(at):
        if 0 < at <= len(rounds):
            pl.semaphore_wait(chain.at[at - 1], 2)
        if at < len(rounds):
            for way in (1, -1):
                pl.semaphore_signal(
                    chain.at[at],
                    inc=1,
                    device_id={"gx": ring(way * rounds[at])},
                    device_id_type=MESH,
                )

    chain_step(0)

    def prepare():
        i = lax.broadcasted_iota(jnp.int32, (128, 512), 0)
        n = lax.broadcasted_iota(jnp.int32, (128, 512), 1)
        lane = n % 128
        expand[...] = (i == (n // 128) * 32 + (lane // 64) * 16 + (lane % 32) // 2).astype(F32)
        n = lax.broadcasted_iota(jnp.int32, (512, 128), 0)
        o = lax.broadcasted_iota(jnp.int32, (512, 128), 1)
        lane = n % 128
        gather[...] = jnp.where(
            o == (n // 128) * 32 + (lane // 64) * 16 + (lane % 32) // 2, 0.125, 0.0
        )
        loads[2].wait()
        for x in range(16):
            rows = pl.ds(x * 32, 32)
            d = 6.0 + diag[rows, :]
            diag[rows, :] = d
            weight[rows, :] = OMEGA / d
        loads[4].wait()
        for X in range(32):
            rows = pl.ds(X * 32, 32)
            d = 6.0 + fdiag[rows, :]
            fdiag[rows, :] = d
            fweight[rows, :] = OMEGA / d
        for at in (1, 3, 5):
            loads[at].wait()

    norm_row = lax.broadcasted_iota(jnp.int32, (1, 128), 1)

    def norm_copy(src, dst, sem, device):
        return pltpu.make_async_remote_copy(
            src_ref=src,
            dst_ref=dst,
            send_sem=n_sem.at[sem],
            recv_sem=n_sem.at[sem + 1],
            device_id=device,
            device_id_type=MESH,
        )

    def send_norms():
        parts = [jnp.sum(csum[k] + fsum[k]) for k in range(CYCLES)]
        row = jnp.where(norm_row < 64, parts[0], parts[1])
        n_send[0] = row
        nx_in[gx] = row

        for i in sorted(range(1, n_x), key=lambda d: -min(d, n_x - d)):
            norm_copy(n_send.at[0], nx_in.at[gx], 0, {"gx": lax.rem(gx + i, n_x)}).start()

    def turn_norms():
        part = nx_in.at[pl.ds(0, n_x - 1)]
        pltpu.make_async_copy(part, part, n_sem.at[1]).wait()
        row = nx_in[0]
        for r in range(1, n_x):
            row = row + nx_in[r]
        n_send[1] = row
        np_in[me] = row

        def send(q):
            norm_copy(n_send.at[1], np_in.at[me], 2, peer(q)).start()

        for q in others():
            send(q)

    def end_norms():
        wait_all(np_in, n_sem.at[3])
        row = np_in[0]
        for r in range(1, members):
            row = row + np_in[r]
        row = jnp.sqrt(row / cells)
        for k in range(CYCLES):
            norm_out[k] = row[0, 64 * k]

    def cycle(c, carry):
        use_parents(c)
        for k in range(CYCLES):

            @pl.when(c == k)
            def _(k=k):
                chain_step(2 * k + 1)

        fine_sweeps(c)
        send_restricted(c)
        for k in range(CYCLES):

            @pl.when(c == k)
            def _(k=k):
                chain_step(2 * k + 2)

        recv_restricted(c)

        def sweep(s, carry):
            coarse_sweep(c, c * CSWEEPS + s, False)
            coarse_inner(c * CSWEEPS + s + 1)
            return carry

        lax.fori_loop(0, CSWEEPS - 1, sweep, 0)
        coarse_sweep(c, c * CSWEEPS + CSWEEPS - 1, True)

        @pl.when(c == CYCLES - 1)
        def _():
            send_norms()

        send_parents(c)
        coarse_inner(c * CSWEEPS + CSWEEPS)
        recv_parents(c)
        return carry

    prepare()
    coarse_inner(0)
    recv_surfaces()
    lax.fori_loop(0, CYCLES, cycle, 0)

    pot_out[...] = pot[SWEEPS]
    live = ((row32 % 4).astype(F32) < jnp.concatenate([count[...]] * 4, axis=0)).astype(F32)
    end = CYCLES % 2
    for X in range(32):
        rows = pl.ds(X * 32, 32)
        fine_out[rows, :] = (fine[end, rows, :] + ghost[pl.ds(X // 2 * 32, 32), :]) * live
    turn_norms()

    wait_all(s_out, s_sem.at[0])
    for c in range(CYCLES):
        wait_all(d_out.at[c], d_send.at[c])
        wait_all(r_out.at[c], r_send.at[c])
    halo(SWEEPS, range(6), "recv")

    def left(k, carry):
        halo(k, range(6), "send")
        return carry

    lax.fori_loop(0, SWEEPS + 1, left, 0)
    part = nx_in.at[pl.ds(0, n_x - 1)]
    pltpu.make_async_copy(part, part, n_sem.at[0]).wait()
    end_norms()
    wait_all(np_in, n_sem.at[2])


def local(
    coarse_source,
    coarse_shift,
    coarse_start,
    fine_source,
    fine_shift,
    fine_start,
    box_corner,
    box_owner,
):
    n_x, n_y, n_z = (lax.axis_size(a) for a in ("gx", "gy", "gz"))
    members = n_y * n_z
    cells = float(n_x * n_y * n_z * coarse_source.size)

    def fine_rows(array):
        return array.reshape(SLOTS, 256, 128).transpose(1, 0, 2).reshape(FROWS, 128)

    hbm = pl.BlockSpec(memory_space=pltpu.HBM)
    smem = pl.BlockSpec(memory_space=pltpu.SMEM)
    vmem = pl.BlockSpec(memory_space=pltpu.VMEM)

    def buf(*shape):
        return pltpu.VMEM(shape, F32)

    sems = pltpu.SemaphoreType.DMA
    pot, fine, norms = pl.pallas_call(
        functools.partial(kernel, (n_x, n_y, n_z, cells)),
        out_shape=(
            jax.ShapeDtypeStruct((ROWS, 128), F32),
            jax.ShapeDtypeStruct((FROWS, 128), F32),
            jax.ShapeDtypeStruct((CYCLES,), F32),
        ),
        in_specs=[hbm] * 8,
        out_specs=(vmem, vmem, smem),
        scratch_shapes=[
            buf(SWEEPS + 1, ROWS, 128),
            buf(ROWS, 128),
            buf(ROWS, 128),
            buf(ROWS, 128),
            buf(ROWS, 128),
            buf(ROWS, 128),
            buf(SWEEPS + 1, 32, 128),
            buf(SWEEPS + 1, 32, 128),
            buf(SWEEPS + 1, 16, 128),
            buf(SWEEPS + 1, 16, 128),
            buf(SWEEPS + 1, 8, 128),
            buf(SWEEPS + 1, 8, 128),
            buf(SWEEPS + 1, 2, 16, 128),
            buf(SWEEPS + 1, 8, 128),
            buf(2, FROWS, 128),
            buf(FROWS, 128),
            buf(FROWS, 128),
            buf(FROWS, 128),
            buf(128, 512),
            buf(512, 128),
            buf(128, 128),
            buf(ROWS, 128),
            buf(128, 512),
            buf(SLOTS, 32, 128),
            pltpu.VMEM((2, 256, 384), jnp.bfloat16),
            buf(SLOTS, 256, 128),
            pltpu.VMEM((SLOTS, 384, 128), jnp.bfloat16),
            pltpu.VMEM((SLOTS, 384, 128), jnp.bfloat16),
            buf(8 * PITCH, 128),
            buf(SLOTS, 32, 128),
            buf(members, 8, 128),
            buf(8, 128),
            pltpu.SMEM((3, 1, SLOTS), jnp.int32),
            pltpu.SMEM((1, SLOTS), jnp.int32),
            pltpu.SMEM((members,), jnp.int32),
            pltpu.SMEM((members,), jnp.int32),
            buf(SLOTS, 12, 128),
            buf(members, 12, 128),
            buf(members, 12, 128),
            buf(CYCLES, members, 32, 128),
            buf(CYCLES, members, 32, 128),
            buf(CYCLES, members, 32, 128),
            buf(CYCLES, members, 32, 128),
            buf(CYCLES, 8, 128),
            buf(CYCLES, 8, 128),
            buf(n_x, 1, 128),
            buf(members, 1, 128),
            buf(2, 1, 128),
            sems((8,)),
            sems((2,)),
            sems((CYCLES,)),
            sems((CYCLES,)),
            sems((CYCLES,)),
            sems((CYCLES,)),
            sems((SWEEPS + 1, 6)),
            sems((SWEEPS + 1, 6)),
            sems((4,)),
            pltpu.SemaphoreType.REGULAR((4,)),
        ],
        compiler_params=pltpu.CompilerParams(
            collective_id=0, has_side_effects=True, vmem_limit_bytes=30 * 1000 * 1000
        ),
        name="cycles",
    )(
        *(
            pltpu.with_memory_space_constraint(array, pltpu.HBM)
            for array in (
                box_corner.transpose(2, 0, 1),
                box_owner,
                coarse_source.reshape(ROWS, 128),
                coarse_shift.reshape(ROWS, 128),
                coarse_start.reshape(ROWS, 128),
                fine_rows(fine_source),
                fine_rows(fine_shift),
                fine_rows(fine_start),
            )
        ),
    )
    fine = fine.reshape(256, SLOTS, 128).transpose(1, 0, 2).reshape(SLOTS, 256 * 128)
    return pot.reshape(coarse_source.shape), fine, norms


def solution(mesh):
    every = ("gx", "gy", "gz")
    return jax.shard_map(
        local,
        mesh=mesh,
        in_specs=(
            P("gx", "gy", "gz"),
            P("gx", "gy", "gz"),
            P("gx", "gy", "gz"),
            P(every, None),
            P(every, None),
            P(every, None),
            P(every, None, None),
            P(every, None),
        ),
        out_specs=(P("gx", "gy", "gz"), P(every, None), P()),
        check_vma=False,
    )
```
